32 devices in a mesh: dp: 8 (over y, x, core), tensor: 4 (over z).
Axes of the slice: x: 2, y: 2, z: 4, core: 2. Of those that a mesh axis runs over, the one named last changes fastest.
Arguments:
- node_features: bfloat16 [8192, 768], P(('dp', 'tensor')), may hold values from -6 to 6
- graph_ids: int32 [64, 128], P('dp'), may hold values from 0 to 5, never falling along the last dimension, each value on 1 to 32 neighbouring positions
- degree: int32 [8192], P(('dp', 'tensor')), may hold values from 0 to 511
- distance: int32 [8192, 128], P('dp'), may hold values from 0 to 511
- out_grad: bfloat16 [8192, 768], P(('dp', 'tensor')), may hold values from -6 to 6
- qkv_weight: bfloat16 [3, 768, 768], P(None, 'tensor'), may hold values from -0.21875 to 0.21875
- qv_bias: float32 [2, 768], P(None, 'tensor'), may hold values from -3 to 3
- out_weight: bfloat16 [768, 768], P('tensor'), may hold values from -0.625 to 0.625
- out_bias: float32 [768], replicated, may hold values from -3 to 3
- norm1_gain: float32 [768], replicated, may hold values from 0.5 to 1.5
- norm1_shift: float32 [768], replicated, may hold values from -2 to 2
- ffn_in_weight: bfloat16 [768, 768], P('tensor'), may hold values from -0.21875 to 0.21875
- ffn_in_bias: float32 [768], P('tensor'), may hold values from -3 to 3
- ffn_out_weight: bfloat16 [768, 768], P('tensor'), may hold values from -0.21875 to 0.21875
- ffn_out_bias: float32 [768], replicated, may hold values from -3 to 3
- norm2_gain: float32 [768], replicated, may hold values from 0.5 to 1.5
- norm2_shift: float32 [768], replicated, may hold values from -2 to 2
- degree_table: bfloat16 [512, 768], replicated, may hold values from -3 to 3
- spatial_table: bfloat16 [32, 512], P('tensor'), may hold values from -4 to 4
Outputs:
- layer_out: bfloat16 [8192, 768], P(('dp', 'tensor'))
- input_grad: bfloat16 [8192, 768], P(('dp', 'tensor'))
- qkv_weight_grad: float32 [3, 768, 768], P(None, 'tensor')
- qv_bias_grad: float32 [2, 768], P(None, 'tensor')
- out_weight_grad: float32 [768, 768], P('tensor')
- out_bias_grad: float32 [768], replicated
- norm1_gain_grad: float32 [768], replicated
- norm1_shift_grad: float32 [768], replicated
- ffn_in_weight_grad: float32 [768, 768], P('tensor')
- ffn_in_bias_grad: float32 [768], P('tensor')
- ffn_out_weight_grad: float32 [768, 768], P('tensor')
- ffn_out_bias_grad: float32 [768], replicated
- norm2_gain_grad: float32 [768], replicated
- norm2_shift_grad: float32 [768], replicated
- degree_table_grad: float32 [512, 768], replicated
- spatial_table_grad: float32 [32, 512], P('tensor')
The draws below stay inside these ranges and needn't reach their ends.
Inputs may be any that keep to these rules, and one draw needn't show every extreme that they name: `graph_ids`: graph numbers never fall along a packed block; a graph holds at most a quarter of 128 nodes, and in every block some graph holds exactly that many.
All inputs are finite; a program needn't handle non-finite values.
Results may differ from the reference program's by a relative error of at most 0.018.
Values may be sent and summed in bfloat16 or wider, within the bound.
A program may use at most 128 MiB of HBM per device.

```python
import math
import jax
import jax.numpy as jnp
import numpy as np
from jax import lax

D = 768
HEADS = 32
FF = 768
NDEG = 512
NSPD = 512
BLOCK = 128
HEAD_DIM = 24
BLOCKS = 64
NODES = 8192


def with_ends(entries, stream_key, least, largest):
    dims = entries.shape
    index_at = [jax.random.randint(jax.random.fold_in(stream_key, axis), (), 0, dims[axis]) for axis in range(len(dims))]
    entries = entries.at[tuple(index_at)].set(least)
    longest = dims.index(max(dims))
    index_at[longest] = (index_at[longest] + 1) % dims[longest]
    return entries.at[tuple(index_at)].set(largest)


def steps_of(key, extent, split, low, largest):
    def one(position, blocks):
        steps = jax.random.uniform(jax.random.fold_in(jax.random.fold_in(key, 6), position), (blocks,), jnp.float32, low / len(split), largest / len(split))
        return jnp.repeat(jnp.exp(steps), extent[position] // blocks).reshape((-1,) + (1,) * (len(extent) - position - 1))

    loudness = one(*split[0])
    for cut in split[1:]:
        loudness = loudness * one(*cut)
    return loudness


def profile(amount, total, most, skew):
    weights = [(1 << 20) // math.isqrt(standing ** skew) + 1 for standing in range(2, amount + 1)]
    rest, counts = total - most - (amount - 1), [1] * (amount - 1)
    while rest > 0:
        candidates = [i for i in range(amount - 1) if counts[i] < most]
        pool, left = sum([weights[i] for i in candidates]), rest
        for i in candidates:
            extra = min(most - counts[i], max(1, left * weights[i] // pool), rest)
            counts[i] = counts[i] + extra
            rest = rest - extra
    return np.array([most] + counts)


def uneven(own_key, amount, total, reach, slope):
    if amount == 2:
        one = jax.random.randint(own_key, (), max(1, total - reach), min(reach, total - 1) + 1)
        return jnp.stack([one, total - one])
    sizes = jnp.asarray(profile(amount, total, reach, slope), jnp.int32)
    twos = (amount - 1) // 2
    donor, sink = sizes[1:1 + 2 * twos:2], sizes[2:2 + 2 * twos:2]
    margin = jnp.minimum(donor - 1, reach - sink)
    moved = jax.random.randint(jax.random.fold_in(own_key, 1), (twos,), 0, 1 << 20) % (margin + 1)
    sizes = sizes.at[1:1 + 2 * twos:2].set(donor - moved).at[2:2 + 2 * twos:2].set(sink + moved)
    return sizes[jax.random.permutation(jax.random.fold_in(own_key, 2), amount)]


def centred(rng, shape, scale, limit, split=(), kind=jnp.bfloat16):
    drawn = scale * jax.random.normal(rng, shape, jnp.float32)
    if split:
        drawn = drawn * steps_of(rng, shape, split, -0.22, 0.18)
    return jnp.clip(drawn, -limit, limit).astype(kind)


def setup_inputs(seed: int = 0) -> dict:
    splits = jax.random.split(jax.random.key(seed), 20)
    return {
        "node_features": centred(splits[0], (NODES, D), 1.0, 6.0, ((0, 32),)),
        "graph_ids": jax.vmap(lambda own: jnp.searchsorted(jnp.cumsum(uneven(own, 6, BLOCK, BLOCK // 4, 0)), jnp.arange(BLOCK), side="right"))(jax.random.split(splits[1], BLOCKS)).reshape((BLOCKS, BLOCK)).astype(jnp.int32),
        "degree": with_ends(jax.random.randint(splits[2], (NODES,), 0, NDEG), jax.random.fold_in(splits[2], 1), 0, NDEG - 1).astype(jnp.int32),
        "distance": with_ends(jax.random.randint(splits[3], (NODES, BLOCK), 0, NSPD), jax.random.fold_in(splits[3], 1), 0, NSPD - 1).astype(jnp.int32),
        "out_grad": centred(splits[4], (NODES, D), 1.0, 6.0, ((0, 32),)),
        "qkv_weight": centred(splits[5], (3, D, D), D ** -0.5, 0.21875, ((1, 4),)),
        "qv_bias": centred(splits[6], (2, D), 0.5, 3.0, ((1, 4),), jnp.float32),
        "out_weight": centred(splits[7], (D, D), (D // 8) ** -0.5, 0.625, ((0, 4),)),
        "out_bias": centred(splits[8], (D,), 0.5, 3.0, (), jnp.float32),
        "norm1_gain": jnp.clip(1.0 + 0.1 * jax.random.normal(splits[9], (D,), jnp.float32), 0.5, 1.5),
        "norm1_shift": centred(splits[10], (D,), 0.3, 2.0, (), jnp.float32),
        "ffn_in_weight": centred(splits[11], (FF, D), D ** -0.5, 0.21875, ((0, 4),)),
        "ffn_in_bias": centred(splits[12], (FF,), 0.5, 3.0, ((0, 4),), jnp.float32),
        "ffn_out_weight": centred(splits[13], (FF, D), FF ** -0.5, 0.21875, ((0, 4),)),
        "ffn_out_bias": centred(splits[14], (D,), 0.5, 3.0, (), jnp.float32),
        "norm2_gain": jnp.clip(1.0 + 0.1 * jax.random.normal(splits[15], (D,), jnp.float32), 0.5, 1.5),
        "norm2_shift": centred(splits[16], (D,), 0.3, 2.0, (), jnp.float32),
        "degree_table": centred(splits[17], (NDEG, D), 0.5, 3.0),
        "spatial_table": centred(splits[18], (HEADS, NSPD), 1.0, 4.0, ((0, 4),)),
    }


norm_eps = 1e-05
masked_score = -1e+30
highest = lax.Precision.HIGHEST

@jax.custom_vjp
def low(v):
    return lax.optimization_barrier(v.astype(jnp.bfloat16)).astype(jnp.float32)

@jax.custom_vjp
def low_back(v):
    return v

def low_keep(v):
    return (low(v), None)

def low_pass(kept, grad):
    return (grad,)

def back_keep(v):
    return (v, None)

def back_low(kept, grad):
    return (low(grad),)
low.defvjp(low_keep, low_pass)
low_back.defvjp(back_keep, back_low)

def layer_norm(hidden_rows, gain, shift):
    row_mean = lax.optimization_barrier(jnp.mean(hidden_rows, axis=-1, keepdims=True))
    centered = hidden_rows - row_mean
    variance = lax.optimization_barrier(jnp.mean(centered * centered, axis=-1, keepdims=True))
    return centered * lax.rsqrt(variance + norm_eps) * gain + shift

def span_forward(params, features, graph_rows, degree_rows, distance_rows):
    qkv_weight, qv_bias, out_weight, out_bias, norm1_gain, norm1_shift, ffn_in_weight, ffn_in_bias, ffn_out_weight, ffn_out_bias, norm2_gain, norm2_shift, degree_table, spatial_table = params
    row_count = features.shape[0]
    block_count = graph_rows.shape[0]
    score_scale = 1.0 / math.sqrt(HEAD_DIM)
    embedded = features + degree_table[degree_rows]
    normed1 = low(layer_norm(embedded, norm1_gain, norm1_shift))
    projected = jnp.dot(normed1, qkv_weight.reshape(3 * D, D).T, precision=highest).reshape(row_count, 3, D)
    head_shape = (block_count, BLOCK, HEADS, HEAD_DIM)
    query = low_back(low(projected[:, 0] + qv_bias[0])).reshape(head_shape)
    keys = low_back(low(projected[:, 1])).reshape(head_shape)
    values = low_back(low(projected[:, 2] + qv_bias[1])).reshape(head_shape)
    pair_bias = jnp.transpose(spatial_table[:, distance_rows.reshape(block_count, BLOCK, BLOCK)], (1, 0, 2, 3))
    raw_scores = jnp.einsum('bihd,bjhd->bhij', query, keys, precision=highest) * score_scale + pair_bias
    scores = low_back(raw_scores)
    same_graph = (graph_rows[:, :, None] == graph_rows[:, None, :])[:, None]
    scores = jnp.where(same_graph, scores, masked_score)
    shifted = jnp.exp(scores - lax.optimization_barrier(jnp.max(scores, axis=-1, keepdims=True)))
    probs = low(shifted / lax.optimization_barrier(jnp.sum(shifted, axis=-1, keepdims=True)))
    mixed = low_back(low(jnp.einsum('bhij,bjhd->bihd', probs, values, precision=highest))).reshape(row_count, D)
    residual1 = embedded + low_back(jnp.dot(mixed, out_weight, precision=highest)) + out_bias
    normed2 = low(layer_norm(residual1, norm2_gain, norm2_shift))
    pre_act = low_back(jnp.dot(normed2, ffn_in_weight.T, precision=highest) + ffn_in_bias)
    hidden = low(jax.nn.gelu(pre_act, approximate=False))
    return residual1 + low_back(jnp.dot(hidden, ffn_out_weight, precision=highest)) + ffn_out_bias

def reference(node_features, graph_ids, degree, distance, out_grad, qkv_weight, qv_bias, out_weight, out_bias, norm1_gain, norm1_shift, ffn_in_weight, ffn_in_bias, ffn_out_weight, ffn_out_bias, norm2_gain, norm2_shift, degree_table, spatial_table):
    params = (qkv_weight.astype(jnp.float32), qv_bias.astype(jnp.float32), out_weight.astype(jnp.float32), out_bias.astype(jnp.float32), norm1_gain.astype(jnp.float32), norm1_shift.astype(jnp.float32), ffn_in_weight.astype(jnp.float32), ffn_in_bias.astype(jnp.float32), ffn_out_weight.astype(jnp.float32), ffn_out_bias.astype(jnp.float32), norm2_gain.astype(jnp.float32), norm2_shift.astype(jnp.float32), degree_table.astype(jnp.float32), spatial_table.astype(jnp.float32))
    span_blocks = math.gcd(BLOCKS, 32)
    span_count = BLOCKS // span_blocks
    span_rows = span_blocks * BLOCK
    graph_spans = graph_ids.reshape(span_count, span_blocks, BLOCK)
    degree_spans = degree.reshape(span_count, span_rows)
    distance_spans = distance.reshape(span_count, span_rows, BLOCK)
    stepper = jax.checkpoint(span_forward)

    def whole_layer(features, weights):

        def one_span(pieces):
            return stepper(weights, pieces[0], pieces[1], pieces[2], pieces[3])
        outputs = lax.map(one_span, (features.reshape(span_count, span_rows, D), graph_spans, degree_spans, distance_spans))
        return outputs.reshape(NODES, D)
    layer_value, pull_back = jax.vjp(whole_layer, node_features.astype(jnp.float32), params)
    input_grad, weight_grads = pull_back(out_grad.astype(jnp.float32))
    qkv_grad, qv_grad, out_w_grad, out_b_grad, gain1_grad, shift1_grad, ffn_in_grad, ffn_in_b_grad, ffn_out_grad, ffn_out_b_grad, gain2_grad, shift2_grad, degree_grad, spatial_grad = weight_grads
    return (layer_value.astype(jnp.bfloat16), input_grad.astype(jnp.bfloat16), qkv_grad, qv_grad, out_w_grad, out_b_grad, gain1_grad, shift1_grad, ffn_in_grad, ffn_in_b_grad, ffn_out_grad, ffn_out_b_grad, gain2_grad, shift2_grad, degree_grad, spatial_grad)
```

```python
import functools
import math

import jax
import jax.numpy as jnp
from jax import lax
from jax.experimental import pallas as pl
from jax.experimental.pallas import tpu as pltpu
from jax.sharding import PartitionSpec as P

norm_eps = 1e-05
masked_score = -1e30
MESH = pl.DeviceIdType.MESH
WEIGHTS = 6


def norm_rows(hidden_rows, gain, shift):
    row_mean = jnp.mean(hidden_rows, axis=1, keepdims=True)
    centered = hidden_rows - row_mean
    variance = jnp.mean(centered * centered, axis=1, keepdims=True)
    inverse = lax.rsqrt(variance + norm_eps)
    normed = centered * inverse
    return (normed, inverse, (normed * gain + shift).astype(jnp.bfloat16))


def norm_back(upstream, normed, inverse, gain):
    scaled = upstream * gain
    first_mean = jnp.mean(scaled, axis=1, keepdims=True)
    second_mean = jnp.mean(scaled * normed, axis=1, keepdims=True)
    through = inverse * (scaled - first_mean - normed * second_mean)
    return (through, jnp.sum(upstream * normed, axis=0), jnp.sum(upstream, axis=0))


def inner_rows(left, right):
    return lax.dot_general(
        left, right, (((0,), (0,)), ((), ())), preferred_element_type=jnp.float32
    )


def against_cols(left, right):
    return lax.dot_general(
        left, right, (((1,), (1,)), ((), ())), preferred_element_type=jnp.float32
    )


def place():
    dp = lax.axis_index("dp")
    tensor = lax.axis_index("tensor")
    core = lax.rem(dp, 2)
    bit_x = lax.rem(dp // 2, 2)
    bit_y = lax.rem(dp // 4, 2)
    return dp, tensor, core, bit_x, bit_y


def partners(dp, core, bit_x, bit_y):
    return dp + 1 - 2 * core, dp + 2 - 4 * bit_x, dp + 4 - 8 * bit_y


def greet(devices):
    barrier = pltpu.get_barrier_semaphore()
    for device in devices:
        pl.semaphore_signal(barrier, inc=1, device_id=device, device_id_type=MESH)
    pl.semaphore_wait(barrier, len(devices))


def send(source, target, send_sem, recv_sem, device):
    copy = pltpu.make_async_remote_copy(
        src_ref=source,
        dst_ref=target,
        send_sem=send_sem,
        recv_sem=recv_sem,
        device_id=device,
        device_id_type=MESH,
    )
    copy.start()
    return copy


def gather_kernel(
    planes,
    half,
    qkv,
    out_w,
    in_w,
    ffn_w,
    table,
    bias,
    full,
    tables,
    biases,
    send_sem,
    recv_sem,
    small_send,
    small_recv,
    own_sem,
):
    dp, tensor, core, bit_x, bit_y = place()
    across_core, across_x, across_y = partners(dp, core, bit_x, bit_y)
    greet(
        [(across_core, tensor), (across_x, tensor), (across_y, tensor)]
        + [(dp, lax.rem(tensor + k, planes)) for k in range(1, planes)]
    )
    lanes = pl.ds(pl.multiple_of(core * half, half), half)
    shards = [qkv.at[0], qkv.at[1], qkv.at[2], out_w, in_w, ffn_w]
    started = []
    small = []
    for k in range(1, planes):
        other = lax.rem(tensor + k, planes)
        for n, (own, whole) in enumerate(((table, tables), (bias, biases))):
            small.append(
                send(
                    own,
                    whole.at[tensor],
                    small_send.at[n, k - 1],
                    small_recv.at[n, k - 1],
                    (dp, other),
                )
            )
    locals_ = [
        pltpu.make_async_copy(table, tables.at[tensor], own_sem.at[WEIGHTS]),
        pltpu.make_async_copy(bias, biases.at[tensor], own_sem.at[WEIGHTS + 1]),
    ]
    stage_z, stage_a, stage_b, stage_c = {}, {}, {}, {}
    for w in range(WEIGHTS):
        first, second = (bit_x, bit_y) if w % 2 == 0 else (bit_y, bit_x)
        for k in range(1, planes):
            other = lax.rem(tensor + k, planes)
            stage_z[w, k] = send(
                shards[w].at[first, second, :, lanes],
                full.at[w, tensor, first, second, :, lanes],
                send_sem.at[0, w, k - 1],
                recv_sem.at[0, w, k - 1],
                (dp, other),
            )
    for w in range(WEIGHTS):
        locals_.append(pltpu.make_async_copy(shards[w], full.at[w, tensor], own_sem.at[w]))
    for copy in locals_:
        copy.start()
    for w in range(WEIGHTS):
        first, second = (bit_x, bit_y) if w % 2 == 0 else (bit_y, bit_x)
        across = across_y if w % 2 == 0 else across_x
        for k in range(1, planes):
            stage_z[w, k].wait_recv()
            whose = lax.rem(tensor + planes - k, planes)
            region = full.at[w, whose, first, second, :, lanes]
            stage_a[w, k] = send(
                region, region, send_sem.at[1, w, k - 1], recv_sem.at[1, w, k - 1], (across, tensor)
            )
    for w in range(WEIGHTS):
        first = bit_x if w % 2 == 0 else bit_y
        across = across_x if w % 2 == 0 else across_y
        for k in range(1, planes):
            stage_a[w, k].wait_recv()
            whose = lax.rem(tensor + planes - k, planes)
            region = full.at[w, whose, first, :, :, lanes]
            stage_b[w, k] = send(
                region, region, send_sem.at[2, w, k - 1], recv_sem.at[2, w, k - 1], (across, tensor)
            )
    for w in range(WEIGHTS):
        for k in range(1, planes):
            stage_b[w, k].wait_recv()
            whose = lax.rem(tensor + planes - k, planes)
            region = full.at[w, whose, :, :, :, lanes]
            stage_c[w, k] = send(
                region,
                region,
                send_sem.at[3, w, k - 1],
                recv_sem.at[3, w, k - 1],
                (across_core, tensor),
            )
    for copy in small:
        copy.wait_recv()
    for copy in stage_c.values():
        copy.wait_recv()
    for copy in locals_:
        copy.wait()
    for stage in (stage_z, stage_a, stage_b, stage_c):
        for copy in stage.values():
            copy.wait_send()
    for copy in small:
        copy.wait_send()


def gather_weights(planes, qkv, out_w, in_w, ffn_w, table, bias):
    shard_rows, width = out_w.shape
    part = shard_rows // 4
    half = width // 2

    def split(matrix):
        return matrix.reshape(matrix.shape[:-2] + (2, 2, part, width))

    vmem = pl.BlockSpec(memory_space=pltpu.VMEM)
    full, tables, biases = pl.pallas_call(
        functools.partial(gather_kernel, planes, half),
        out_shape=(
            jax.ShapeDtypeStruct((WEIGHTS, planes, 2, 2, part, width), jnp.bfloat16),
            jax.ShapeDtypeStruct((planes,) + table.shape, jnp.bfloat16),
            jax.ShapeDtypeStruct((planes,) + bias.shape, jnp.float32),
        ),
        in_specs=[vmem] * 6,
        out_specs=(vmem,) * 3,
        scratch_shapes=[
            pltpu.SemaphoreType.DMA((4, WEIGHTS, planes - 1)),
            pltpu.SemaphoreType.DMA((4, WEIGHTS, planes - 1)),
            pltpu.SemaphoreType.DMA((2, planes - 1)),
            pltpu.SemaphoreType.DMA((2, planes - 1)),
            pltpu.SemaphoreType.DMA((WEIGHTS + 2,)),
        ],
        compiler_params=pltpu.CompilerParams(collective_id=0, has_side_effects=True),
        name="gather_weights",
    )(split(qkv), split(out_w), split(in_w), split(ffn_w), table, bias)
    return (
        full.reshape(WEIGHTS, planes * shard_rows, width),
        tables.reshape(-1, table.shape[1]),
        biases.transpose(1, 0, 2).reshape(bias.shape[0], -1),
    )


def add_into(target, left, right):
    target[...] = (left[...].astype(jnp.float32) + right[...].astype(jnp.float32)).astype(target.dtype)


def reduce_kernel(
    planes,
    groups,
    grads,
    table,
    small,
    fin,
    fin_table,
    fin_small,
    recv_c,
    recv_a,
    recv_b,
    recv_z,
    recv_g,
    sum_c,
    sum_a,
    sum_b,
    trecv_c,
    trecv_a,
    trecv_b,
    trecv_z,
    trecv_g,
    tsum_c,
    tsum_a,
    tsum_b,
    srecv_c,
    srecv_a,
    srecv_b,
    srecv_z,
    srecv_g,
    ssum_a,
    ssum_b,
    ssum_z,
    ssum_g,
    send_sem,
    recv_sem,
):
    dp, tensor, core, bit_x, bit_y = place()
    across_core, across_x, across_y = partners(dp, core, bit_x, bit_y)
    group = dp // 8
    rest = [lax.rem(group + k, groups) * 8 + lax.rem(dp, 8) for k in range(1, groups)]
    greet(
        [(across_core, tensor), (across_x, tensor), (across_y, tensor)]
        + [(dp, lax.rem(tensor + k, planes)) for k in range(1, planes)]
        + [(other, tensor) for other in rest]
    )
    jobs = []
    copies = []
    counter = [0]

    def push(source, target, device):
        n = counter[0]
        counter[0] += 1
        copy = send(source, target, send_sem.at[n], recv_sem.at[n], device)
        copies.append(copy)
        return copy

    def small_job():
        copy = push(small, srecv_c, (across_core, tensor))
        yield
        copy.wait_recv()
        add_into(ssum_a, small, srecv_c)
        copy = push(ssum_a, srecv_a, (across_x, tensor))
        yield
        copy.wait_recv()
        add_into(ssum_b, ssum_a, srecv_a)
        copy = push(ssum_b, srecv_b, (across_y, tensor))
        yield
        copy.wait_recv()
        add_into(ssum_z, ssum_b, srecv_b)
        srecv_z[tensor] = ssum_z[...]
        sent = [
            push(ssum_z, srecv_z.at[tensor], (dp, lax.rem(tensor + k, planes)))
            for k in range(1, planes)
        ]
        yield
        for copy in sent:
            copy.wait_recv()
        total = srecv_z[0].astype(jnp.float32)
        for k in range(1, planes):
            total = total + srecv_z[k].astype(jnp.float32)
        if groups > 1:
            ssum_g[...] = total.astype(jnp.bfloat16)
            srecv_g[group] = ssum_g[...]
            sent = [push(ssum_g, srecv_g.at[group], (other, tensor)) for other in rest]
            for copy in sent:
                copy.wait_recv()
            total = srecv_g[0].astype(jnp.float32)
            for k in range(1, groups):
                total = total + srecv_g[k].astype(jnp.float32)
        fin_small[...] = total

    def matrix_job(w, whole, parts, bufs, spread):
        c_in, a_in, b_in, z_in, g_in, c_sum, a_sum, b_sum = bufs
        x_first = w % 2 == 0
        first, second = (bit_x, bit_y) if x_first else (bit_y, bit_x)
        to_first, to_second = (across_x, across_y) if x_first else (across_y, across_x)
        copy = push(whole.at[1 - core], c_in, (across_core, tensor))
        yield
        copy.wait_recv()
        own = whole.at[core]
        for p in range(planes):
            add_into(c_sum.at[:, :, p], own.at[:, :, p], c_in.at[:, :, p])
        copy = push(c_sum.at[1 - first], a_in, (to_first, tensor))
        yield
        copy.wait_recv()
        for q in range(2):
            add_into(a_sum.at[q], c_sum.at[first, q], a_in.at[q])
        copy = push(a_sum.at[1 - second], b_in, (to_second, tensor))
        yield
        copy.wait_recv()
        add_into(b_sum, a_sum.at[second], b_in)
        sent = []
        for k in range(1, planes):
            other = lax.rem(tensor + k, planes)
            sent.append(push(b_sum.at[other], z_in.at[k - 1], (dp, other)))
        yield
        for copy in sent:
            copy.wait_recv()
        total = b_sum[tensor].astype(jnp.float32)
        for k in range(1, planes):
            total = total + z_in[k - 1].astype(jnp.float32)
        mine = parts.at[core, first, second, tensor] if spread else parts.at[core, first, second]
        mine[...] = total.astype(jnp.bfloat16)
        if groups > 1:
            g_in[group] = mine[...]
            sent = [push(mine, g_in.at[group], (other, tensor)) for other in rest]
            for copy in sent:
                copy.wait_recv()
            total = g_in[0].astype(jnp.float32)
            for k in range(1, groups):
                total = total + g_in[k].astype(jnp.float32)
            for copy in sent:
                copy.wait_send()
            mine[...] = total.astype(jnp.bfloat16)
        if spread:
            sent = [
                push(mine, mine, (dp, lax.rem(tensor + k, planes))) for k in range(1, planes)
            ]
            yield
            for copy in sent:
                copy.wait_recv()
        region = parts.at[core, first, second]
        copy = push(region, region, (to_second, tensor))
        yield
        copy.wait_recv()
        region = parts.at[core, first]
        copy = push(region, region, (to_first, tensor))
        yield
        copy.wait_recv()
        region = parts.at[core]
        copy = push(region, region, (across_core, tensor))
        yield
        copy.wait_recv()

    jobs.append(small_job())
    jobs.append(
        matrix_job(
            0,
            table,
            fin_table,
            (trecv_c, trecv_a, trecv_b, trecv_z, trecv_g, tsum_c, tsum_a, tsum_b),
            True,
        )
    )
    for w in range(WEIGHTS):
        jobs.append(
            matrix_job(
                w,
                grads.at[w],
                fin.at[w],
                (
                    recv_c.at[w],
                    recv_a.at[w],
                    recv_b.at[w],
                    recv_z.at[w],
                    recv_g.at[w] if groups > 1 else None,
                    sum_c.at[w],
                    sum_a.at[w],
                    sum_b.at[w],
                ),
                False,
            )
        )
    while jobs:
        left = []
        for job in jobs:
            try:
                next(job)
                left.append(job)
            except StopIteration:
                pass
        jobs = left
    for copy in copies:
        copy.wait_send()


def reduce_all(planes, groups, grads, table, small):
    part, half = grads.shape[-2:]
    tpart = table.shape[-2]
    bf = jnp.bfloat16
    vmem = pl.BlockSpec(memory_space=pltpu.VMEM)
    spare = max(groups, 1)

    def many(lead, rows):
        return [
            pltpu.VMEM(lead + (2, 2, planes, rows, half), bf),
            pltpu.VMEM(lead + (2, planes, rows, half), bf),
            pltpu.VMEM(lead + (planes, rows, half), bf),
            pltpu.VMEM(lead + (planes - 1, rows, half), bf),
            pltpu.VMEM(lead + (spare, rows, half), bf),
            pltpu.VMEM(lead + (2, 2, planes, rows, half), bf),
            pltpu.VMEM(lead + (2, planes, rows, half), bf),
            pltpu.VMEM(lead + (planes, rows, half), bf),
        ]

    small_buf = pltpu.VMEM(small.shape, bf)
    rest = groups - 1
    sends = WEIGHTS * (6 + planes - 1 + rest) + (6 + 2 * (planes - 1) + rest) + 3 + planes - 1 + rest
    return pl.pallas_call(
        functools.partial(reduce_kernel, planes, groups),
        out_shape=(
            jax.ShapeDtypeStruct((WEIGHTS, 2, 2, 2, part, half), bf),
            jax.ShapeDtypeStruct((2, 2, 2, planes, tpart, half), bf),
            jax.ShapeDtypeStruct(small.shape, jnp.float32),
        ),
        in_specs=[vmem] * 3,
        out_specs=(vmem,) * 3,
        scratch_shapes=many((WEIGHTS,), part)
        + many((), tpart)
        + [
            small_buf,
            small_buf,
            small_buf,
            pltpu.VMEM((planes,) + small.shape, bf),
            pltpu.VMEM((spare,) + small.shape, bf),
            small_buf,
            small_buf,
            small_buf,
            small_buf,
            pltpu.SemaphoreType.DMA((sends,)),
            pltpu.SemaphoreType.DMA((sends,)),
        ],
        compiler_params=pltpu.CompilerParams(collective_id=1, has_side_effects=True),
        name="reduce_grads",
    )(grads, table, small)


def blocked(matrix, planes):
    rows, width = matrix.shape
    part = rows // (planes * 4)
    return matrix.reshape(planes, 2, 2, part, 2, width // 2).transpose(4, 1, 2, 0, 3, 5)


def shards(
    planes,
    groups,
    node_features,
    graph_ids,
    degree,
    distance,
    out_grad,
    qkv_weight,
    qv_bias,
    out_weight,
    out_bias,
    norm1_gain,
    norm1_shift,
    ffn_in_weight,
    ffn_in_bias,
    ffn_out_weight,
    ffn_out_bias,
    norm2_gain,
    norm2_shift,
    degree_table,
    spatial_table,
):
    tensor = lax.axis_index("tensor")
    rows = node_features.shape[0]
    block_size = graph_ids.shape[1]
    blocks = rows // block_size
    local_width = qkv_weight.shape[1]
    width = qkv_weight.shape[2]
    heads = spatial_table.shape[0] * planes
    table_rows = spatial_table.shape[1]
    head_dim = width // heads
    score_scale = 1.0 / math.sqrt(head_dim)

    bias_pack = jnp.concatenate([qv_bias, ffn_in_bias[None]], axis=0)
    weights, whole_table, whole_bias = gather_weights(
        planes, qkv_weight, out_weight, ffn_in_weight, ffn_out_weight, spatial_table, bias_pack
    )
    graph_rows = lax.dynamic_slice_in_dim(graph_ids, tensor * blocks, blocks, 0)
    distances = lax.dynamic_slice_in_dim(distance, tensor * rows, rows, 0)

    degree_onehot = (
        degree[:, None] == lax.broadcasted_iota(jnp.int32, (1, degree_table.shape[0]), 1)
    ).astype(jnp.bfloat16)
    embedded = node_features.astype(jnp.float32) + jnp.dot(
        degree_onehot, degree_table, preferred_element_type=jnp.float32
    )
    normed1, inverse1, act1 = norm_rows(embedded, norm1_gain, norm1_shift)
    projected = against_cols(act1, weights[:3].reshape(3 * width, width)).reshape(rows, 3, width)
    query = (projected[:, 0] + whole_bias[0]).astype(jnp.bfloat16)
    keys = projected[:, 1].astype(jnp.bfloat16)
    values = (projected[:, 2] + whole_bias[1]).astype(jnp.bfloat16)

    flat = distances.reshape(1, -1)
    onehot = (lax.broadcasted_iota(jnp.int32, (table_rows, flat.shape[1]), 0) == flat).astype(
        jnp.bfloat16
    )
    bias = (
        jnp.dot(whole_table, onehot, preferred_element_type=jnp.float32)
        .reshape(heads, blocks, block_size, block_size)
        .transpose(1, 0, 2, 3)
    )

    def headed(matrix):
        return matrix.reshape(blocks, block_size, heads, head_dim)

    q, k, v = headed(query), headed(keys), headed(values)
    raw = (
        jnp.einsum("bihd,bjhd->bhij", q, k, preferred_element_type=jnp.float32) * score_scale + bias
    )
    same = (graph_rows[:, :, None] == graph_rows[:, None, :])[:, None]
    scores = jnp.where(same, raw, masked_score)
    shifted = jnp.exp(scores - jnp.max(scores, axis=-1, keepdims=True))
    soft = shifted / jnp.sum(shifted, axis=-1, keepdims=True)
    probs = soft.astype(jnp.bfloat16)
    mixed = (
        jnp.einsum("bhij,bjhd->bihd", probs, v, preferred_element_type=jnp.float32)
        .reshape(rows, width)
        .astype(jnp.bfloat16)
    )
    residual1 = embedded + jnp.dot(mixed, weights[3], preferred_element_type=jnp.float32) + out_bias
    normed2, inverse2, act2 = norm_rows(residual1, norm2_gain, norm2_shift)
    pre_act = against_cols(act2, weights[4]) + whole_bias[2]
    hidden = jax.nn.gelu(pre_act, approximate=False).astype(jnp.bfloat16)
    layer_out = (
        residual1 + jnp.dot(hidden, weights[5], preferred_element_type=jnp.float32) + ffn_out_bias
    ).astype(jnp.bfloat16)

    upstream = out_grad.astype(jnp.float32)
    ffn_out_grad = inner_rows(hidden, out_grad)
    hidden_grad = against_cols(out_grad, weights[5])
    unused_value, gelu_pull = jax.vjp(
        lambda pre_value: jax.nn.gelu(pre_value, approximate=False), pre_act
    )
    pre_grad = gelu_pull(hidden_grad)[0].astype(jnp.bfloat16)
    ffn_in_grad = inner_rows(pre_grad, act2)
    normed2_grad = jnp.dot(pre_grad, weights[4], preferred_element_type=jnp.float32)
    through2, norm2_gain_grad, norm2_shift_grad = norm_back(
        normed2_grad, normed2, inverse2, norm2_gain
    )
    residual1_grad = upstream + through2
    attn_grad = residual1_grad.astype(jnp.bfloat16)
    out_weight_grad = inner_rows(mixed, attn_grad)
    mixed_grad = headed(against_cols(attn_grad, weights[3]).astype(jnp.bfloat16))
    values_grad = jnp.einsum(
        "bhij,bihd->bjhd", probs, mixed_grad, preferred_element_type=jnp.float32
    )
    probs_grad = jnp.einsum(
        "bihd,bjhd->bhij", mixed_grad, v, preferred_element_type=jnp.float32
    )
    scores_grad = (
        soft * (probs_grad - jnp.sum(soft * probs_grad, axis=-1, keepdims=True))
    ).astype(jnp.bfloat16)
    query_grad = (
        jnp.einsum("bhij,bjhd->bihd", scores_grad, k, preferred_element_type=jnp.float32)
        * score_scale
    )
    keys_grad = (
        jnp.einsum("bhij,bihd->bjhd", scores_grad, q, preferred_element_type=jnp.float32)
        * score_scale
    )
    stacked = jnp.concatenate(
        [piece.reshape(rows, width) for piece in (query_grad, keys_grad, values_grad)], axis=1
    ).astype(jnp.bfloat16)
    qkv_grad = inner_rows(stacked, act1).reshape(3, width, width)
    normed1_grad = jnp.dot(
        stacked, weights[:3].reshape(3 * width, width), preferred_element_type=jnp.float32
    )
    spatial_grad = against_cols(scores_grad.transpose(1, 0, 2, 3).reshape(heads, -1), onehot)
    through1, norm1_gain_grad, norm1_shift_grad = norm_back(
        normed1_grad, normed1, inverse1, norm1_gain
    )
    embedded_grad = residual1_grad + through1
    input_grad = embedded_grad.astype(jnp.bfloat16)
    grad_lower = (embedded_grad - input_grad.astype(jnp.float32)).astype(jnp.bfloat16)
    degree_grad = inner_rows(degree_onehot, input_grad) + inner_rows(degree_onehot, grad_lower)

    stacked_float = stacked.astype(jnp.float32)
    vectors = jnp.stack(
        [
            jnp.sum(stacked_float[:, :width], axis=0),
            jnp.sum(stacked_float[:, 2 * width :], axis=0),
            jnp.sum(pre_grad.astype(jnp.float32), axis=0),
            jnp.sum(residual1_grad, axis=0),
            norm1_gain_grad,
            norm1_shift_grad,
            jnp.sum(upstream, axis=0),
            norm2_gain_grad,
            norm2_shift_grad,
        ]
    )
    small_rows = -(-(heads + vectors.shape[0]) // 16) * 16
    small = jnp.zeros((small_rows, width), jnp.float32)
    small = small.at[:heads, :table_rows].set(spatial_grad)
    small = small.at[heads : heads + vectors.shape[0]].set(vectors).astype(jnp.bfloat16)
    low = [
        blocked(grad.astype(jnp.bfloat16), planes)
        for grad in (qkv_grad[0], qkv_grad[1], qkv_grad[2], out_weight_grad, ffn_in_grad, ffn_out_grad)
    ]
    fin, fin_table, total = reduce_all(
        planes, groups, jnp.stack(low), blocked(degree_grad.astype(jnp.bfloat16), planes), small
    )

    def shard_of(piece):
        return piece.transpose(1, 2, 3, 0, 4).reshape(local_width, width).astype(jnp.float32)

    finished = [shard_of(fin[w]) for w in range(WEIGHTS)]
    table_grad = (
        fin_table.transpose(3, 1, 2, 4, 0, 5).reshape(degree_table.shape).astype(jnp.float32)
    )
    local_heads = spatial_table.shape[0]
    spatial_out = lax.dynamic_slice(
        total, (tensor * local_heads, 0), (local_heads, table_rows)
    )
    tail = total[heads : heads + vectors.shape[0]]
    local = lax.dynamic_slice(tail, (0, tensor * local_width), (3, local_width))
    return (
        layer_out,
        input_grad,
        jnp.stack(finished[:3]),
        local[:2],
        finished[3],
        tail[3],
        tail[4],
        tail[5],
        finished[4],
        local[2],
        finished[5],
        tail[6],
        tail[7],
        tail[8],
        table_grad,
        spatial_out,
    )


def solution(mesh):
    planes = mesh.shape["tensor"]
    groups = mesh.shape["dp"] // 8
    return jax.shard_map(
        functools.partial(shards, planes, groups),
        mesh=mesh,
        in_specs=(
            P(("dp", "tensor"), None),
            P("dp", None),
            P(("dp", "tensor")),
            P("dp", None),
            P(("dp", "tensor"), None),
            P(None, "tensor", None),
            P(None, "tensor"),
            P("tensor", None),
            P(),
            P(),
            P(),
            P("tensor", None),
            P("tensor"),
            P("tensor", None),
            P(),
            P(),
            P(),
            P(),
            P("tensor", None),
        ),
        out_specs=(
            P(("dp", "tensor"), None),
            P(("dp", "tensor"), None),
            P(None, "tensor", None),
            P(None, "tensor"),
            P("tensor", None),
            P(),
            P(),
            P(),
            P("tensor", None),
            P("tensor"),
            P("tensor", None),
            P(),
            P(),
            P(),
            P(),
            P("tensor", None),
        ),
        check_vma=False,
    )
```

```python
import functools
import math

import jax
import jax.numpy as jnp
from jax import lax
from jax.experimental import pallas as pl
from jax.experimental.pallas import tpu as pltpu
from jax.sharding import PartitionSpec as P

norm_eps = 1e-05
masked_score = -1e30
MESH = pl.DeviceIdType.MESH
WEIGHTS = 6


def against_cols(left, right):
    return lax.dot_general(
        left, right, (((1,), (1,)), ((), ())), preferred_element_type=jnp.float32
    )


def place():
    dp = lax.axis_index("dp")
    tensor = lax.axis_index("tensor")
    core = lax.rem(dp, 2)
    bit_x = lax.rem(dp // 2, 2)
    bit_y = lax.rem(dp // 4, 2)
    return dp, tensor, core, bit_x, bit_y


def partners(dp, core, bit_x, bit_y):
    return dp + 1 - 2 * core, dp + 2 - 4 * bit_x, dp + 4 - 8 * bit_y


def greet(devices):
    barrier = pltpu.get_barrier_semaphore()
    for device in devices:
        pl.semaphore_signal(barrier, inc=1, device_id=device, device_id_type=MESH)
    pl.semaphore_wait(barrier, len(devices))


def send(source, target, send_sem, recv_sem, device):
    copy = pltpu.make_async_remote_copy(
        src_ref=source,
        dst_ref=target,
        send_sem=send_sem,
        recv_sem=recv_sem,
        device_id=device,
        device_id_type=MESH,
    )
    copy.start()
    return copy


def gather_kernel(
    planes,
    half,
    qkv,
    out_w,
    in_w,
    ffn_w,
    table,
    bias,
    full,
    tables,
    biases,
    send_sem,
    recv_sem,
    small_send,
    small_recv,
    own_sem,
):
    dp, tensor, core, bit_x, bit_y = place()
    across_core, across_x, across_y = partners(dp, core, bit_x, bit_y)
    greet(
        [(across_core, tensor), (across_x, tensor), (across_y, tensor)]
        + [(dp, lax.rem(tensor + k, planes)) for k in range(1, planes)]
    )
    lanes = pl.ds(pl.multiple_of(core * half, half), half)
    shards = [qkv.at[0], qkv.at[1], qkv.at[2], out_w, in_w, ffn_w]
    started = []
    small = []
    for k in range(1, planes):
        other = lax.rem(tensor + k, planes)
        for n, (own, whole) in enumerate(((table, tables), (bias, biases))):
            small.append(
                send(
                    own,
                    whole.at[tensor],
                    small_send.at[n, k - 1],
                    small_recv.at[n, k - 1],
                    (dp, other),
                )
            )
    locals_ = [
        pltpu.make_async_copy(table, tables.at[tensor], own_sem.at[WEIGHTS]),
        pltpu.make_async_copy(bias, biases.at[tensor], own_sem.at[WEIGHTS + 1]),
    ]
    stage_z, stage_a, stage_b, stage_c = {}, {}, {}, {}
    for w in range(WEIGHTS):
        first, second = (bit_x, bit_y) if w % 2 == 0 else (bit_y, bit_x)
        for k in range(1, planes):
            other = lax.rem(tensor + k, planes)
            stage_z[w, k] = send(
                shards[w].at[first, second, :, lanes],
                full.at[w, tensor, first, second, :, lanes],
                send_sem.at[0, w, k - 1],
                recv_sem.at[0, w, k - 1],
                (dp, other),
            )
    for w in range(WEIGHTS):
        locals_.append(pltpu.make_async_copy(shards[w], full.at[w, tensor], own_sem.at[w]))
    for copy in locals_:
        copy.start()
    for w in range(WEIGHTS):
        first, second = (bit_x, bit_y) if w % 2 == 0 else (bit_y, bit_x)
        across = across_y if w % 2 == 0 else across_x
        for k in range(1, planes):
            stage_z[w, k].wait_recv()
            whose = lax.rem(tensor + planes - k, planes)
            region = full.at[w, whose, first, second, :, lanes]
            stage_a[w, k] = send(
                region, region, send_sem.at[1, w, k - 1], recv_sem.at[1, w, k - 1], (across, tensor)
            )
    for w in range(WEIGHTS):
        first = bit_x if w % 2 == 0 else bit_y
        across = across_x if w % 2 == 0 else across_y
        for k in range(1, planes):
            stage_a[w, k].wait_recv()
            whose = lax.rem(tensor + planes - k, planes)
            region = full.at[w, whose, first, :, :, lanes]
            stage_b[w, k] = send(
                region, region, send_sem.at[2, w, k - 1], recv_sem.at[2, w, k - 1], (across, tensor)
            )
    for w in range(WEIGHTS):
        for k in range(1, planes):
            stage_b[w, k].wait_recv()
            whose = lax.rem(tensor + planes - k, planes)
            region = full.at[w, whose, :, :, :, lanes]
            stage_c[w, k] = send(
                region,
                region,
                send_sem.at[3, w, k - 1],
                recv_sem.at[3, w, k - 1],
                (across_core, tensor),
            )
    for copy in small:
        copy.wait_recv()
    for copy in stage_c.values():
        copy.wait_recv()
    for copy in locals_:
        copy.wait()
    for stage in (stage_z, stage_a, stage_b, stage_c):
        for copy in stage.values():
            copy.wait_send()
    for copy in small:
        copy.wait_send()


def gather_weights(planes, qkv, out_w, in_w, ffn_w, table, bias):
    shard_rows, width = out_w.shape
    part = shard_rows // 4
    half = width // 2

    def split(matrix):
        return matrix.reshape(matrix.shape[:-2] + (2, 2, part, width))

    vmem = pl.BlockSpec(memory_space=pltpu.VMEM)
    full, tables, biases = pl.pallas_call(
        functools.partial(gather_kernel, planes, half),
        out_shape=(
            jax.ShapeDtypeStruct((WEIGHTS, planes, 2, 2, part, width), jnp.bfloat16),
            jax.ShapeDtypeStruct((planes,) + table.shape, jnp.bfloat16),
            jax.ShapeDtypeStruct((planes,) + bias.shape, jnp.float32),
        ),
        in_specs=[vmem] * 6,
        out_specs=(vmem,) * 3,
        scratch_shapes=[
            pltpu.SemaphoreType.DMA((4, WEIGHTS, planes - 1)),
            pltpu.SemaphoreType.DMA((4, WEIGHTS, planes - 1)),
            pltpu.SemaphoreType.DMA((2, planes - 1)),
            pltpu.SemaphoreType.DMA((2, planes - 1)),
            pltpu.SemaphoreType.DMA((WEIGHTS + 2,)),
        ],
        compiler_params=pltpu.CompilerParams(collective_id=0, has_side_effects=True),
        name="gather_weights",
    )(split(qkv), split(out_w), split(in_w), split(ffn_w), table, bias)
    return (
        full.reshape(WEIGHTS, planes * shard_rows, width),
        tables.reshape(-1, table.shape[1]),
        biases.transpose(1, 0, 2).reshape(bias.shape[0], -1),
    )


def add_into(target, left, right):
    target[...] = (left[...].astype(jnp.float32) + right[...].astype(jnp.float32)).astype(target.dtype)


def reduce_kernel(
    planes,
    groups,
    grads,
    table,
    small,
    fin,
    fin_table,
    fin_small,
    recv_c,
    recv_a,
    recv_b,
    recv_z,
    recv_g,
    sum_c,
    sum_a,
    sum_b,
    trecv_c,
    trecv_a,
    trecv_b,
    trecv_z,
    trecv_g,
    tsum_c,
    tsum_a,
    tsum_b,
    srecv_c,
    srecv_a,
    srecv_b,
    srecv_z,
    srecv_g,
    ssum_a,
    ssum_b,
    ssum_z,
    ssum_g,
    send_sem,
    recv_sem,
):
    dp, tensor, core, bit_x, bit_y = place()
    across_core, across_x, across_y = partners(dp, core, bit_x, bit_y)
    group = dp // 8
    rest = [lax.rem(group + k, groups) * 8 + lax.rem(dp, 8) for k in range(1, groups)]
    greet(
        [(across_core, tensor), (across_x, tensor), (across_y, tensor)]
        + [(dp, lax.rem(tensor + k, planes)) for k in range(1, planes)]
        + [(other, tensor) for other in rest]
    )
    jobs = []
    copies = []
    counter = [0]

    def push(source, target, device):
        n = counter[0]
        counter[0] += 1
        copy = send(source, target, send_sem.at[n], recv_sem.at[n], device)
        copies.append(copy)
        return copy

    def small_job():
        copy = push(small, srecv_c, (across_core, tensor))
        yield
        copy.wait_recv()
        add_into(ssum_a, small, srecv_c)
        copy = push(ssum_a, srecv_a, (across_x, tensor))
        yield
        copy.wait_recv()
        add_into(ssum_b, ssum_a, srecv_a)
        copy = push(ssum_b, srecv_b, (across_y, tensor))
        yield
        copy.wait_recv()
        add_into(ssum_z, ssum_b, srecv_b)
        srecv_z[tensor] = ssum_z[...]
        sent = [
            push(ssum_z, srecv_z.at[tensor], (dp, lax.rem(tensor + k, planes)))
            for k in range(1, planes)
        ]
        yield
        for copy in sent:
            copy.wait_recv()
        total = srecv_z[0].astype(jnp.float32)
        for k in range(1, planes):
            total = total + srecv_z[k].astype(jnp.float32)
        if groups > 1:
            ssum_g[...] = total.astype(jnp.bfloat16)
            srecv_g[group] = ssum_g[...]
            sent = [push(ssum_g, srecv_g.at[group], (other, tensor)) for other in rest]
            for copy in sent:
                copy.wait_recv()
            total = srecv_g[0].astype(jnp.float32)
            for k in range(1, groups):
                total = total + srecv_g[k].astype(jnp.float32)
        fin_small[...] = total

    def matrix_job(w, whole, parts, bufs, spread):
        c_in, a_in, b_in, z_in, g_in, c_sum, a_sum, b_sum = bufs
        x_first = w % 2 == 0
        first, second = (bit_x, bit_y) if x_first else (bit_y, bit_x)
        to_first, to_second = (across_x, across_y) if x_first else (across_y, across_x)
        copy = push(whole.at[1 - core], c_in, (across_core, tensor))
        yield
        copy.wait_recv()
        own = whole.at[core]
        for p in range(planes):
            add_into(c_sum.at[:, :, p], own.at[:, :, p], c_in.at[:, :, p])
        copy = push(c_sum.at[1 - first], a_in, (to_first, tensor))
        yield
        copy.wait_recv()
        for q in range(2):
            add_into(a_sum.at[q], c_sum.at[first, q], a_in.at[q])
        copy = push(a_sum.at[1 - second], b_in, (to_second, tensor))
        yield
        copy.wait_recv()
        add_into(b_sum, a_sum.at[second], b_in)
        sent = []
        for k in range(1, planes):
            other = lax.rem(tensor + k, planes)
            sent.append(push(b_sum.at[other], z_in.at[k - 1], (dp, other)))
        yield
        for copy in sent:
            copy.wait_recv()
        total = b_sum[tensor].astype(jnp.float32)
        for k in range(1, planes):
            total = total + z_in[k - 1].astype(jnp.float32)
        mine = parts.at[core, first, second, tensor] if spread else parts.at[core, first, second]
        mine[...] = total.astype(jnp.bfloat16)
        if groups > 1:
            g_in[group] = mine[...]
            sent = [push(mine, g_in.at[group], (other, tensor)) for other in rest]
            for copy in sent:
                copy.wait_recv()
            total = g_in[0].astype(jnp.float32)
            for k in range(1, groups):
                total = total + g_in[k].astype(jnp.float32)
            for copy in sent:
                copy.wait_send()
            mine[...] = total.astype(jnp.bfloat16)
        if spread:
            sent = [
                push(mine, mine, (dp, lax.rem(tensor + k, planes))) for k in range(1, planes)
            ]
            yield
            for copy in sent:
                copy.wait_recv()
        region = parts.at[core, first, second]
        copy = push(region, region, (to_second, tensor))
        yield
        copy.wait_recv()
        region = parts.at[core, first]
        copy = push(region, region, (to_first, tensor))
        yield
        copy.wait_recv()
        region = parts.at[core]
        copy = push(region, region, (across_core, tensor))
        yield
        copy.wait_recv()

    jobs.append(small_job())
    jobs.append(
        matrix_job(
            0,
            table,
            fin_table,
            (trecv_c, trecv_a, trecv_b, trecv_z, trecv_g, tsum_c, tsum_a, tsum_b),
            True,
        )
    )
    for w in range(WEIGHTS):
        jobs.append(
            matrix_job(
                w,
                grads.at[w],
                fin.at[w],
                (
                    recv_c.at[w],
                    recv_a.at[w],
                    recv_b.at[w],
                    recv_z.at[w],
                    recv_g.at[w] if groups > 1 else None,
                    sum_c.at[w],
                    sum_a.at[w],
                    sum_b.at[w],
                ),
                False,
            )
        )
    while jobs:
        left = []
        for job in jobs:
            try:
                next(job)
                left.append(job)
            except StopIteration:
                pass
        jobs = left
    for copy in copies:
        copy.wait_send()


def reduce_all(planes, groups, grads, table, small):
    part, half = grads.shape[-2:]
    tpart = table.shape[-2]
    bf = jnp.bfloat16
    vmem = pl.BlockSpec(memory_space=pltpu.VMEM)
    spare = max(groups, 1)

    def many(lead, rows):
        return [
            pltpu.VMEM(lead + (2, 2, planes, rows, half), bf),
            pltpu.VMEM(lead + (2, planes, rows, half), bf),
            pltpu.VMEM(lead + (planes, rows, half), bf),
            pltpu.VMEM(lead + (planes - 1, rows, half), bf),
            pltpu.VMEM(lead + (spare, rows, half), bf),
            pltpu.VMEM(lead + (2, 2, planes, rows, half), bf),
            pltpu.VMEM(lead + (2, planes, rows, half), bf),
            pltpu.VMEM(lead + (planes, rows, half), bf),
        ]

    small_buf = pltpu.VMEM(small.shape, bf)
    rest = groups - 1
    sends = WEIGHTS * (6 + planes - 1 + rest) + (6 + 2 * (planes - 1) + rest) + 3 + planes - 1 + rest
    return pl.pallas_call(
        functools.partial(reduce_kernel, planes, groups),
        out_shape=(
            jax.ShapeDtypeStruct((WEIGHTS, 2, 2, 2, part, half), bf),
            jax.ShapeDtypeStruct((2, 2, 2, planes, tpart, half), bf),
            jax.ShapeDtypeStruct(small.shape, jnp.float32),
        ),
        in_specs=[vmem] * 3,
        out_specs=(vmem,) * 3,
        scratch_shapes=many((WEIGHTS,), part)
        + many((), tpart)
        + [
            small_buf,
            small_buf,
            small_buf,
            pltpu.VMEM((planes,) + small.shape, bf),
            pltpu.VMEM((spare,) + small.shape, bf),
            small_buf,
            small_buf,
            small_buf,
            small_buf,
            pltpu.SemaphoreType.DMA((sends,)),
            pltpu.SemaphoreType.DMA((sends,)),
        ],
        compiler_params=pltpu.CompilerParams(collective_id=1, has_side_effects=True),
        name="reduce_grads",
    )(grads, table, small)


def transposed_left(left, right):
    return lax.dot_general(
        left, right, (((0,), (0,)), ((), ())), preferred_element_type=jnp.float32
    )


def plain(left, right):
    return lax.dot_general(
        left, right, (((1,), (0,)), ((), ())), preferred_element_type=jnp.float32
    )


def normalized(rows):
    row_mean = jnp.mean(rows, axis=1, keepdims=True)
    centered = rows - row_mean
    variance = jnp.mean(centered * centered, axis=1, keepdims=True)
    inverse = lax.rsqrt(variance + norm_eps)
    return centered * inverse, inverse


def layer_kernel(
    shape,
    features,
    graph_ids,
    degree,
    distance,
    out_grad,
    weights,
    table,
    bias,
    vectors,
    degree_table,
    layer_out,
    input_grad,
    grads,
    table_grad,
    small,
    embedded,
    normed,
    act,
    qkv,
    mixed,
    soft,
    scores_grad,
    fold_low,
    fold_high,
    fold_same,
    residual,
    second,
    act2,
    mixed_grad,
    stacked,
    pre_act,
    bias_cols,
):
    planes, heads, head_dim, block, half = shape
    rows, width = features.shape
    blocks = rows // block
    fold = block // 2
    scale = 1.0 / math.sqrt(head_dim)
    bf = jnp.bfloat16
    f32 = jnp.float32
    tensor = lax.axis_index("tensor")
    out_bias, gain1, shift1, ffn_bias, gain2, shift2 = (vectors[pl.ds(n, 1), :] for n in range(6))

    onehot = (
        lax.broadcasted_iota(jnp.int32, (degree_table.shape[0], rows), 0) == degree[...]
    ).astype(f32).astype(bf)
    embedded[...] = features[...].astype(f32) + transposed_left(onehot, degree_table[...])
    first, inverse1 = normalized(embedded[...])
    normed[...] = first
    act[...] = (first * gain1 + shift1).astype(bf)

    position = lax.broadcasted_iota(jnp.int32, (fold, block), 0)
    lane = lax.broadcasted_iota(jnp.int32, (fold, block), 1)
    inside = jnp.abs(lane - position) < block // 4

    def folded(square):
        return jnp.where(inside, square[:fold], square[fold:])

    def unfolded(part):
        zero = jnp.zeros_like(part)
        return jnp.concatenate(
            [jnp.where(inside, part, zero), jnp.where(inside, zero, part)], axis=0
        ).astype(bf)

    for g in range(blocks):
        start = pl.multiple_of(tensor * rows + g * block, block)
        index = folded(jnp.transpose(distance[pl.ds(start, block), :]))
        lanes = pl.ds(g * block, block)
        fold_low[:, lanes] = lax.rem(index, 128)
        fold_high[:, lanes] = index // 128
        across = jnp.broadcast_to(graph_ids[pl.ds(tensor * blocks + g, 1), :], (block, block))
        down = folded(jnp.transpose(across))
        fold_same[:, lanes] = jnp.where(down == across[:fold], 1, 0)

    bias_cols[...] = jnp.transpose(bias[...])
    act_rows = act[...]
    for k in range(3):
        part = against_cols(weights[k], act_rows)
        if k != 1:
            column = 0 if k == 0 else 1
            part = part + bias_cols[:, column : column + 1]
        qkv[k] = part

    def head_rows(h):
        return pl.ds(pl.multiple_of(h * head_dim, 8), head_dim)

    def forward(h, carry):
        for g in range(blocks):
            lanes = pl.ds(g * block, block)
            q = qkv[0, head_rows(h), lanes].astype(bf)
            k = qkv[1, head_rows(h), lanes].astype(bf)
            v = qkv[2, head_rows(h), lanes].astype(bf)
            raw = folded(transposed_left(k, q))
            low = fold_low[:, lanes]
            high = fold_high[:, lanes]
            looked = None
            for c in range(table.shape[1]):
                source = jnp.broadcast_to(table[h, pl.ds(c, 1), :], (fold, 128))
                found = jnp.take_along_axis(source, low, axis=1, mode="promise_in_bounds")
                looked = found if c == 0 else jnp.where(high == c, found, looked)
            scores = jnp.where(fold_same[:, lanes] == 1, raw * scale + looked, masked_score)
            shifted = jnp.exp(scores - jnp.max(scores, axis=0, keepdims=True))
            part = shifted * (1.0 / jnp.sum(shifted, axis=0, keepdims=True))
            soft[g * heads + h] = part
            mixed[head_rows(h), lanes] = plain(v, unfolded(part))
        return carry

    lax.fori_loop(0, heads, forward, 0, unroll=2)

    mixed_low = mixed[...].astype(bf)
    residual[...] = embedded[...] + transposed_left(mixed_low, weights[3]) + out_bias
    again, inverse2 = normalized(residual[...])
    second[...] = again
    act2[...] = (again * gain2 + shift2).astype(bf)
    pre_act[...] = against_cols(act2[...], weights[4]) + bias[pl.ds(2, 1), :]
    upward = pre_act[...]
    bell = 0.5 * (1.0 + lax.erf(upward * (1.0 / math.sqrt(2.0))))
    hidden = (upward * bell).astype(bf)
    layer_out[...] = (residual[...] + plain(hidden, weights[5]) + ffn_bias).astype(bf)
    grad_low = out_grad[...]
    hidden_grad = against_cols(grad_low, weights[5])
    slope = bell + upward * jnp.exp(-0.5 * upward * upward) * (1.0 / math.sqrt(2.0 * math.pi))
    pre_grad = (hidden_grad * slope).astype(bf)

    part = grads.shape[-2]

    def keep(target, matrix, rows_each):
        low = matrix.astype(bf)
        for p in range(planes):
            for a in range(2):
                for b in range(2):
                    at = ((p * 2 + a) * 2 + b) * rows_each
                    for c in range(2):
                        target[c, a, b, p] = low[at : at + rows_each, c * half : (c + 1) * half]

    keep(grads.at[5], transposed_left(hidden, grad_low), part)
    keep(grads.at[4], transposed_left(pre_grad, act2[...]), part)
    small[...] = jnp.zeros_like(small)
    table_width = table.shape[1] * 128

    def note(row, values):
        small[pl.ds(heads + row, 1), :] = values

    def down_sum(values):
        return jnp.sum(values, axis=0, keepdims=True)

    note(2, down_sum(pre_grad.astype(f32)))
    upstream = grad_low.astype(f32)
    note(6, down_sum(upstream))
    normed2_grad = plain(pre_grad, weights[4])

    def norm_through(grad, unit, inverse, gain):
        scaled = grad * gain
        first_mean = jnp.mean(scaled, axis=1, keepdims=True)
        second_mean = jnp.mean(scaled * unit, axis=1, keepdims=True)
        return inverse * (scaled - first_mean - unit * second_mean)

    note(7, down_sum(normed2_grad * second[...]))
    note(8, down_sum(normed2_grad))
    residual_grad = upstream + norm_through(normed2_grad, second[...], inverse2, gain2)
    residual[...] = residual_grad
    note(3, down_sum(residual_grad))
    attn_grad = residual_grad.astype(bf)
    keep(grads.at[3], plain(mixed_low, attn_grad), part)
    mixed_grad[...] = against_cols(weights[3], attn_grad)

    def backward(h, carry):
        for g in range(blocks):
            lanes = pl.ds(g * block, block)
            q = qkv[0, head_rows(h), lanes].astype(bf)
            k = qkv[1, head_rows(h), lanes].astype(bf)
            v = qkv[2, head_rows(h), lanes].astype(bf)
            d = mixed_grad[head_rows(h), lanes].astype(bf)
            probs = soft[g * heads + h]
            weighted = probs * folded(transposed_left(v, d))
            change = weighted - probs * jnp.sum(weighted, axis=0, keepdims=True)
            change_low = change.astype(bf).astype(f32)
            scores_grad[g, pl.ds(h, fold, stride=heads), :] = change_low
            change_full = unfolded(change_low)
            stacked[0, head_rows(h), lanes] = plain(k, change_full) * scale
            stacked[1, head_rows(h), lanes] = against_cols(q, change_full) * scale
            stacked[2, head_rows(h), lanes] = against_cols(d, unfolded(probs))
        return carry

    lax.fori_loop(0, heads, backward, 0, unroll=2)

    def tally(j, total):
        change = jnp.concatenate(
            [scores_grad[g, pl.ds(pl.multiple_of(j * heads, 8), heads), :] for g in range(blocks)],
            axis=1,
        )
        low = fold_low[pl.ds(j, 1), :]
        high = fold_high[pl.ds(j, 1), :]
        picked = jnp.concatenate(
            [jnp.where(high == c, change, 0.0) for c in range(table.shape[1])], axis=0
        ).astype(bf)
        mark = (lax.broadcasted_iota(jnp.int32, (128, rows), 0) == low).astype(f32).astype(bf)
        return total + against_cols(picked, mark)

    tallied = lax.fori_loop(
        0, fold, tally, jnp.zeros((table.shape[1] * heads, 128), f32), unroll=2
    )
    for c in range(table.shape[1]):
        small[pl.ds(0, heads), pl.ds(c * 128, 128)] = tallied[c * heads : (c + 1) * heads]

    normed1_grad = None
    for k in range(3):
        low = stacked[k].astype(bf)
        if k != 1:
            note(0 if k == 0 else 1, down_sum(jnp.transpose(low.astype(f32))))
        keep(grads.at[k], plain(low, act_rows), part)
        piece = transposed_left(low, weights[k])
        normed1_grad = piece if k == 0 else normed1_grad + piece
    note(4, down_sum(normed1_grad * normed[...]))
    note(5, down_sum(normed1_grad))
    embedded_grad = residual[...] + norm_through(normed1_grad, normed[...], inverse1, gain1)
    embedded_low = embedded_grad.astype(bf)
    input_grad[...] = embedded_low
    keep(table_grad, plain(onehot, embedded_low), table_grad.shape[-2])


def run_layer(
    planes, heads, features, graph_ids, degree, distance, out_grad, weights, table, bias, vectors, degree_table
):
    rows, width = features.shape
    block = graph_ids.shape[1]
    blocks = rows // block
    half = width // 2
    part = width // (planes * 4)
    table_part = degree_table.shape[0] // (planes * 4)
    small_rows = -(-(heads + 9) // 16) * 16
    bf, f32 = jnp.bfloat16, jnp.float32
    vmem = pl.BlockSpec(memory_space=pltpu.VMEM)
    return pl.pallas_call(
        functools.partial(layer_kernel, (planes, heads, width // heads, block, half)),
        out_shape=(
            jax.ShapeDtypeStruct((rows, width), bf),
            jax.ShapeDtypeStruct((rows, width), bf),
            jax.ShapeDtypeStruct((WEIGHTS, 2, 2, 2, planes, part, half), bf),
            jax.ShapeDtypeStruct((2, 2, 2, planes, table_part, half), bf),
            jax.ShapeDtypeStruct((small_rows, width), f32),
        ),
        in_specs=[vmem] * 10,
        out_specs=(vmem,) * 5,
        scratch_shapes=[
            pltpu.VMEM((rows, width), f32),
            pltpu.VMEM((rows, width), f32),
            pltpu.VMEM((rows, width), bf),
            pltpu.VMEM((3, width, rows), f32),
            pltpu.VMEM((width, rows), f32),
            pltpu.VMEM((blocks * heads, block // 2, block), f32),
            pltpu.VMEM((blocks, block // 2 * heads, block), f32),
            pltpu.VMEM((block // 2, rows), jnp.int32),
            pltpu.VMEM((block // 2, rows), jnp.int32),
            pltpu.VMEM((block // 2, rows), jnp.int32),
            pltpu.VMEM((rows, width), f32),
            pltpu.VMEM((rows, width), f32),
            pltpu.VMEM((rows, width), bf),
            pltpu.VMEM((width, rows), f32),
            pltpu.VMEM((3, width, rows), f32),
            pltpu.VMEM((rows, width), f32),
            pltpu.VMEM((width, 8), f32),
        ],
        name="layer",
    )(features, graph_ids, degree, distance, out_grad, weights, table, bias, vectors, degree_table)


def shards(
    planes,
    groups,
    node_features,
    graph_ids,
    degree,
    distance,
    out_grad,
    qkv_weight,
    qv_bias,
    out_weight,
    out_bias,
    norm1_gain,
    norm1_shift,
    ffn_in_weight,
    ffn_in_bias,
    ffn_out_weight,
    ffn_out_bias,
    norm2_gain,
    norm2_shift,
    degree_table,
    spatial_table,
):
    tensor = lax.axis_index("tensor")
    rows = node_features.shape[0]
    local_width = qkv_weight.shape[1]
    width = qkv_weight.shape[2]
    heads = spatial_table.shape[0] * planes
    table_rows = spatial_table.shape[1]

    bias_pack = jnp.pad(jnp.concatenate([qv_bias, ffn_in_bias[None]], axis=0), ((0, 5), (0, 0)))
    weights, whole_table, whole_bias = gather_weights(
        planes, qkv_weight, out_weight, ffn_in_weight, ffn_out_weight, spatial_table, bias_pack
    )
    vectors = jnp.stack(
        [out_bias, norm1_gain, norm1_shift, ffn_out_bias, norm2_gain, norm2_shift, out_bias, out_bias]
    )
    layer_out, input_grad, grads, degree_grad, small = run_layer(
        planes,
        heads,
        node_features,
        graph_ids,
        degree.reshape(1, rows),
        distance,
        out_grad,
        weights,
        whole_table.astype(jnp.float32).reshape(heads, table_rows // 128, 128),
        whole_bias,
        vectors,
        degree_table,
    )
    fin, fin_table, total = reduce_all(
        planes, groups, grads, degree_grad, small.astype(jnp.bfloat16)
    )

    def shard_of(piece):
        return piece.transpose(1, 2, 3, 0, 4).reshape(local_width, width).astype(jnp.float32)

    finished = [shard_of(fin[w]) for w in range(WEIGHTS)]
    table_grad = (
        fin_table.transpose(3, 1, 2, 4, 0, 5).reshape(degree_table.shape).astype(jnp.float32)
    )
    local_heads = spatial_table.shape[0]
    spatial_out = lax.dynamic_slice(
        total, (tensor * local_heads, 0), (local_heads, table_rows)
    )
    tail = total[heads : heads + 9]
    local = lax.dynamic_slice(tail, (0, tensor * local_width), (3, local_width))
    return (
        layer_out,
        input_grad,
        jnp.stack(finished[:3]),
        local[:2],
        finished[3],
        tail[3],
        tail[4],
        tail[5],
        finished[4],
        local[2],
        finished[5],
        tail[6],
        tail[7],
        tail[8],
        table_grad,
        spatial_out,
    )


def solution(mesh):
    planes = mesh.shape["tensor"]
    groups = mesh.shape["dp"] // 8
    return jax.shard_map(
        functools.partial(shards, planes, groups),
        mesh=mesh,
        in_specs=(
            P(("dp", "tensor"), None),
            P("dp", None),
            P(("dp", "tensor")),
            P("dp", None),
            P(("dp", "tensor"), None),
            P(None, "tensor", None),
            P(None, "tensor"),
            P("tensor", None),
            P(),
            P(),
            P(),
            P("tensor", None),
            P("tensor"),
            P("tensor", None),
            P(),
            P(),
            P(),
            P(),
            P("tensor", None),
        ),
        out_specs=(
            P(("dp", "tensor"), None),
            P(("dp", "tensor"), None),
            P(None, "tensor", None),
            P(None, "tensor"),
            P("tensor", None),
            P(),
            P(),
            P(),
            P("tensor", None),
            P("tensor"),
            P("tensor", None),
            P(),
            P(),
            P(),
            P(),
            P("tensor", None),
        ),
        check_vma=False,
    )
```

```python
import functools
import math

import jax
import jax.numpy as jnp
from jax import lax
from jax.experimental import pallas as pl
from jax.experimental.pallas import tpu as pltpu
from jax.sharding import PartitionSpec as P

norm_eps = 1e-05
masked_score = -1e30
MESH = pl.DeviceIdType.MESH
WEIGHTS = 6


def against_cols(left, right):
    return lax.dot_general(
        left, right, (((1,), (1,)), ((), ())), preferred_element_type=jnp.float32
    )


def place():
    dp = lax.axis_index("dp")
    tensor = lax.axis_index("tensor")
    core = lax.rem(dp, 2)
    bit_x = lax.rem(dp // 2, 2)
    bit_y = lax.rem(dp // 4, 2)
    return dp, tensor, core, bit_x, bit_y


def partners(dp, core, bit_x, bit_y):
    return dp + 1 - 2 * core, dp + 2 - 4 * bit_x, dp + 4 - 8 * bit_y


def greet(devices):
    barrier = pltpu.get_barrier_semaphore()
    for device in devices:
        pl.semaphore_signal(barrier, inc=1, device_id=device, device_id_type=MESH)
    pl.semaphore_wait(barrier, len(devices))


def send(source, target, send_sem, recv_sem, device):
    copy = pltpu.make_async_remote_copy(
        src_ref=source,
        dst_ref=target,
        send_sem=send_sem,
        recv_sem=recv_sem,
        device_id=device,
        device_id_type=MESH,
    )
    copy.start()
    return copy


def gather_kernel(
    planes,
    half,
    qkv,
    out_w,
    in_w,
    ffn_w,
    table,
    bias,
    full,
    tables,
    biases,
    send_sem,
    recv_sem,
    small_send,
    small_recv,
    own_sem,
):
    dp, tensor, core, bit_x, bit_y = place()
    across_core, across_x, across_y = partners(dp, core, bit_x, bit_y)
    greet(
        [(across_core, tensor), (across_x, tensor), (across_y, tensor)]
        + [(dp, lax.rem(tensor + k, planes)) for k in range(1, planes)]
    )
    lanes = pl.ds(pl.multiple_of(core * half, half), half)
    shards = [qkv.at[0], qkv.at[1], qkv.at[2], out_w, in_w, ffn_w]
    small = []
    for k in range(1, planes):
        other = lax.rem(tensor + k, planes)
        for n, (own, whole) in enumerate(((table, tables), (bias, biases))):
            small.append(
                send(
                    own,
                    whole.at[tensor],
                    small_send.at[n, k - 1],
                    small_recv.at[n, k - 1],
                    (dp, other),
                )
            )
    locals_ = [
        pltpu.make_async_copy(table, tables.at[tensor], own_sem.at[WEIGHTS]),
        pltpu.make_async_copy(bias, biases.at[tensor], own_sem.at[WEIGHTS + 1]),
    ]
    stage_z, stage_a, stage_b, stage_c = {}, {}, {}, {}
    for w in range(WEIGHTS):
        first, second = (bit_x, bit_y) if w % 2 == 0 else (bit_y, bit_x)
        for k in range(1, planes):
            other = lax.rem(tensor + k, planes)
            stage_z[w, k] = send(
                shards[w].at[first, second, :, lanes],
                full.at[w, tensor, first, second, :, lanes],
                send_sem.at[0, w, k - 1],
                recv_sem.at[0, w, k - 1],
                (dp, other),
            )
    for w in range(WEIGHTS):
        locals_.append(pltpu.make_async_copy(shards[w], full.at[w, tensor], own_sem.at[w]))
    for copy in locals_:
        copy.start()
    def to_second(w):
        first, second = (bit_x, bit_y) if w % 2 == 0 else (bit_y, bit_x)
        across = across_y if w % 2 == 0 else across_x
        for k in range(1, planes):
            stage_z[w, k].wait_recv()
            whose = lax.rem(tensor + planes - k, planes)
            region = full.at[w, whose, first, second, :, lanes]
            stage_a[w, k] = send(
                region, region, send_sem.at[1, w, k - 1], recv_sem.at[1, w, k - 1], (across, tensor)
            )

    def to_first(w):
        first = bit_x if w % 2 == 0 else bit_y
        across = across_x if w % 2 == 0 else across_y
        for k in range(1, planes):
            stage_a[w, k].wait_recv()
            whose = lax.rem(tensor + planes - k, planes)
            region = full.at[w, whose, first, :, :, lanes]
            stage_b[w, k] = send(
                region, region, send_sem.at[2, w, k - 1], recv_sem.at[2, w, k - 1], (across, tensor)
            )

    def to_core(w):
        for k in range(1, planes):
            stage_b[w, k].wait_recv()
            whose = lax.rem(tensor + planes - k, planes)
            region = full.at[w, whose, :, :, :, lanes]
            stage_c[w, k] = send(
                region,
                region,
                send_sem.at[3, w, k - 1],
                recv_sem.at[3, w, k - 1],
                (across_core, tensor),
            )

    for step in range(0, WEIGHTS + 4, 2):
        for stage, late in ((to_core, 4), (to_first, 2), (to_second, 0)):
            for w in (step - late, step - late + 1):
                if 0 <= w < WEIGHTS:
                    stage(w)
    for copy in small:
        copy.wait_recv()
    for copy in stage_c.values():
        copy.wait_recv()
    for copy in locals_:
        copy.wait()
    for stage in (stage_z, stage_a, stage_b, stage_c):
        for copy in stage.values():
            copy.wait_send()
    for copy in small:
        copy.wait_send()


def gather_weights(planes, qkv, out_w, in_w, ffn_w, table, bias):
    shard_rows, width = out_w.shape
    part = shard_rows // 4
    half = width // 2

    def split(matrix):
        return matrix.reshape(matrix.shape[:-2] + (2, 2, part, width))

    vmem = pl.BlockSpec(memory_space=pltpu.VMEM)
    full, tables, biases = pl.pallas_call(
        functools.partial(gather_kernel, planes, half),
        out_shape=(
            jax.ShapeDtypeStruct((WEIGHTS, planes, 2, 2, part, width), jnp.bfloat16),
            jax.ShapeDtypeStruct((planes,) + table.shape, jnp.bfloat16),
            jax.ShapeDtypeStruct((planes,) + bias.shape, jnp.float32),
        ),
        in_specs=[vmem] * 6,
        out_specs=(vmem,) * 3,
        scratch_shapes=[
            pltpu.SemaphoreType.DMA((4, WEIGHTS, planes - 1)),
            pltpu.SemaphoreType.DMA((4, WEIGHTS, planes - 1)),
            pltpu.SemaphoreType.DMA((2, planes - 1)),
            pltpu.SemaphoreType.DMA((2, planes - 1)),
            pltpu.SemaphoreType.DMA((WEIGHTS + 2,)),
        ],
        compiler_params=pltpu.CompilerParams(collective_id=0, has_side_effects=True),
        name="gather_weights",
    )(split(qkv), split(out_w), split(in_w), split(ffn_w), table, bias)
    return full.reshape(WEIGHTS, planes * shard_rows, width), tables, biases


def add_into(target, left, right):
    target[...] = (left[...].astype(jnp.float32) + right[...].astype(jnp.float32)).astype(target.dtype)


def reduce_kernel(
    planes,
    groups,
    grads,
    table,
    small,
    fin,
    fin_table,
    fin_small,
    recv_c,
    recv_a,
    recv_b,
    recv_z,
    recv_g,
    sum_c,
    sum_a,
    sum_b,
    trecv_c,
    trecv_a,
    trecv_b,
    trecv_z,
    trecv_g,
    tsum_c,
    tsum_a,
    tsum_b,
    srecv_c,
    srecv_a,
    srecv_b,
    srecv_z,
    srecv_g,
    ssum_a,
    ssum_b,
    ssum_z,
    ssum_g,
    send_sem,
    recv_sem,
):
    dp, tensor, core, bit_x, bit_y = place()
    across_core, across_x, across_y = partners(dp, core, bit_x, bit_y)
    group = dp // 8
    rest = [lax.rem(group + k, groups) * 8 + lax.rem(dp, 8) for k in range(1, groups)]
    greet(
        [(across_core, tensor), (across_x, tensor), (across_y, tensor)]
        + [(dp, lax.rem(tensor + k, planes)) for k in range(1, planes)]
        + [(other, tensor) for other in rest]
    )
    jobs = []
    copies = []
    counter = [0]

    def push(source, target, device):
        n = counter[0]
        counter[0] += 1
        copy = send(source, target, send_sem.at[n], recv_sem.at[n], device)
        copies.append(copy)
        return copy

    def small_job():
        copy = push(small, srecv_c, (across_core, tensor))
        yield True
        copy.wait_recv()
        add_into(ssum_a, small, srecv_c)
        copy = push(ssum_a, srecv_a, (across_x, tensor))
        yield True
        copy.wait_recv()
        add_into(ssum_b, ssum_a, srecv_a)
        copy = push(ssum_b, srecv_b, (across_y, tensor))
        yield True
        copy.wait_recv()
        add_into(ssum_z, ssum_b, srecv_b)
        srecv_z[tensor] = ssum_z[...]
        sent = [
            push(ssum_z, srecv_z.at[tensor], (dp, lax.rem(tensor + k, planes)))
            for k in range(1, planes)
        ]
        yield True
        for copy in sent:
            copy.wait_recv()
        total = srecv_z[0].astype(jnp.float32)
        for k in range(1, planes):
            total = total + srecv_z[k].astype(jnp.float32)
        if groups > 1:
            ssum_g[...] = total.astype(jnp.bfloat16)
            srecv_g[group] = ssum_g[...]
            sent = [push(ssum_g, srecv_g.at[group], (other, tensor)) for other in rest]
            for copy in sent:
                copy.wait_recv()
            total = srecv_g[0].astype(jnp.float32)
            for k in range(1, groups):
                total = total + srecv_g[k].astype(jnp.float32)
        fin_small[...] = total

    def matrix_job(w, whole, parts, bufs, spread):
        c_in, a_in, b_in, z_in, g_in, c_sum, a_sum, b_sum = bufs
        x_first = w % 2 == 0
        first, second = (bit_x, bit_y) if x_first else (bit_y, bit_x)
        to_first, to_second = (across_x, across_y) if x_first else (across_y, across_x)
        copy = push(whole.at[1 - core], c_in, (across_core, tensor))
        yield True
        copy.wait_recv()
        own = whole.at[core]
        for p in range(planes):
            add_into(c_sum.at[:, :, p], own.at[:, :, p], c_in.at[:, :, p])
        copy = push(c_sum.at[1 - first], a_in, (to_first, tensor))
        yield True
        copy.wait_recv()
        for q in range(2):
            add_into(a_sum.at[q], c_sum.at[first, q], a_in.at[q])
        copy = push(a_sum.at[1 - second], b_in, (to_second, tensor))
        yield True
        copy.wait_recv()
        add_into(b_sum, a_sum.at[second], b_in)
        sent = []
        for k in range(1, planes):
            other = lax.rem(tensor + k, planes)
            sent.append(push(b_sum.at[other], z_in.at[k - 1], (dp, other)))
        yield True
        for copy in sent:
            copy.wait_recv()
        total = b_sum[tensor].astype(jnp.float32)
        for k in range(1, planes):
            total = total + z_in[k - 1].astype(jnp.float32)
        mine = parts.at[core, first, second, tensor] if spread else parts.at[core, first, second]
        mine[...] = total.astype(jnp.bfloat16)
        if groups > 1:
            g_in[group] = mine[...]
            sent = [push(mine, g_in.at[group], (other, tensor)) for other in rest]
            for copy in sent:
                copy.wait_recv()
            total = g_in[0].astype(jnp.float32)
            for k in range(1, groups):
                total = total + g_in[k].astype(jnp.float32)
            for copy in sent:
                copy.wait_send()
            mine[...] = total.astype(jnp.bfloat16)
        if spread:
            sent = [
                push(mine, mine, (dp, lax.rem(tensor + k, planes))) for k in range(1, planes)
            ]
            yield True
            for copy in sent:
                copy.wait_recv()
        region = parts.at[core, first, second]
        copy = push(region, region, (to_second, tensor))
        yield True
        copy.wait_recv()
        region = parts.at[core, first]
        copy = push(region, region, (to_first, tensor))
        yield True
        copy.wait_recv()
        region = parts.at[core]
        copy = push(region, region, (across_core, tensor))
        yield True
        copy.wait_recv()

    jobs.append(small_job())
    jobs.append(
        matrix_job(
            0,
            table,
            fin_table,
            (trecv_c, trecv_a, trecv_b, trecv_z, trecv_g, tsum_c, tsum_a, tsum_b),
            True,
        )
    )
    for w in range(WEIGHTS):
        jobs.append(
            matrix_job(
                w,
                grads.at[w],
                fin.at[w],
                (
                    recv_c.at[w],
                    recv_a.at[w],
                    recv_b.at[w],
                    recv_z.at[w],
                    recv_g.at[w] if groups > 1 else None,
                    sum_c.at[w],
                    sum_a.at[w],
                    sum_b.at[w],
                ),
                False,
            )
        )
    waiting, running = jobs, []
    while waiting or running:
        enter = 4 if not running else 2
        running, waiting = running + waiting[:enter], waiting[enter:]
        running = [job for job in running if next(job, None)]
    for copy in copies:
        copy.wait_send()


def reduce_all(planes, groups, grads, table, small):
    part, half = grads.shape[-2:]
    tpart = table.shape[-2]
    bf = jnp.bfloat16
    vmem = pl.BlockSpec(memory_space=pltpu.VMEM)
    spare = max(groups, 1)

    def many(lead, rows):
        return [
            pltpu.VMEM(lead + (2, 2, planes, rows, half), bf),
            pltpu.VMEM(lead + (2, planes, rows, half), bf),
            pltpu.VMEM(lead + (planes, rows, half), bf),
            pltpu.VMEM(lead + (planes - 1, rows, half), bf),
            pltpu.VMEM(lead + (spare, rows, half), bf),
            pltpu.VMEM(lead + (2, 2, planes, rows, half), bf),
            pltpu.VMEM(lead + (2, planes, rows, half), bf),
            pltpu.VMEM(lead + (planes, rows, half), bf),
        ]

    small_buf = pltpu.VMEM(small.shape, bf)
    rest = groups - 1
    sends = WEIGHTS * (6 + planes - 1 + rest) + (6 + 2 * (planes - 1) + rest) + 3 + planes - 1 + rest
    return pl.pallas_call(
        functools.partial(reduce_kernel, planes, groups),
        out_shape=(
            jax.ShapeDtypeStruct((WEIGHTS, 2, 2, 2, part, half), bf),
            jax.ShapeDtypeStruct((2, 2, 2, planes, tpart, half), bf),
            jax.ShapeDtypeStruct(small.shape, jnp.float32),
        ),
        in_specs=[vmem] * 3,
        out_specs=(vmem,) * 3,
        scratch_shapes=many((WEIGHTS,), part)
        + many((), tpart)
        + [
            small_buf,
            small_buf,
            small_buf,
            pltpu.VMEM((planes,) + small.shape, bf),
            pltpu.VMEM((spare,) + small.shape, bf),
            small_buf,
            small_buf,
            small_buf,
            small_buf,
            pltpu.SemaphoreType.DMA((sends,)),
            pltpu.SemaphoreType.DMA((sends,)),
        ],
        compiler_params=pltpu.CompilerParams(collective_id=1, has_side_effects=True),
        name="reduce_grads",
    )(grads, table, small)


def transposed_left(left, right):
    return lax.dot_general(
        left, right, (((0,), (0,)), ((), ())), preferred_element_type=jnp.float32
    )


def plain(left, right):
    return lax.dot_general(
        left, right, (((1,), (0,)), ((), ())), preferred_element_type=jnp.float32
    )


def normalized(rows):
    row_mean = jnp.mean(rows, axis=1, keepdims=True)
    centered = rows - row_mean
    variance = jnp.mean(centered * centered, axis=1, keepdims=True)
    inverse = lax.rsqrt(variance + norm_eps)
    return centered * inverse, inverse


def layer_kernel(
    shape,
    features,
    graph_ids,
    degree,
    distance,
    out_grad,
    weights,
    tables,
    biases,
    out_bias_in,
    gain1_in,
    shift1_in,
    ffn_bias_in,
    gain2_in,
    shift2_in,
    degree_table,
    layer_out,
    input_grad,
    grads,
    table_grad,
    small_out,
    embedded,
    normed,
    act,
    qkv,
    mixed,
    soft,
    scores_grad,
    fold_low,
    fold_high,
    fold_same,
    residual,
    second,
    act2,
    mixed_grad,
    stacked,
    pre_act,
    bias_cols,
    table,
    small,
):
    planes, heads, head_dim, block, half = shape
    rows, width = features.shape
    blocks = rows // block
    fold = block // 2
    scale = 1.0 / math.sqrt(head_dim)
    bf = jnp.bfloat16
    f32 = jnp.float32
    tensor = lax.axis_index("tensor")
    out_bias, gain1, shift1, ffn_bias, gain2, shift2 = (
        given[...].reshape(1, width)
        for given in (out_bias_in, gain1_in, shift1_in, ffn_bias_in, gain2_in, shift2_in)
    )
    local_heads = heads // planes
    for p in range(planes):
        local = tables[p].astype(f32)
        for c in range(table.shape[1]):
            table[pl.ds(p * local_heads, local_heads), c, :] = local[:, c * 128 : (c + 1) * 128]
    bias = jnp.concatenate([biases[p] for p in range(planes)], axis=1)
    lookups = table.shape[1]

    onehot = (
        lax.broadcasted_iota(jnp.int32, (degree_table.shape[0], rows), 0) == degree[...]
    ).astype(f32).astype(bf)
    embedded[...] = features[...].astype(f32) + transposed_left(onehot, degree_table[...])
    first, inverse1 = normalized(embedded[...])
    normed[...] = first
    act[...] = (first * gain1 + shift1).astype(bf)

    position = lax.broadcasted_iota(jnp.int32, (fold, block), 0)
    lane = lax.broadcasted_iota(jnp.int32, (fold, block), 1)
    inside = jnp.abs(lane - position) < block // 4

    def folded(square):
        return jnp.where(inside, square[:fold], square[fold:])

    def unfolded(part):
        zero = jnp.zeros_like(part)
        return jnp.concatenate(
            [jnp.where(inside, part, zero), jnp.where(inside, zero, part)], axis=0
        ).astype(bf)

    for g in range(blocks):
        start = pl.multiple_of(tensor * rows + g * block, block)
        index = folded(jnp.transpose(distance[pl.ds(start, block), :]))
        lanes = pl.ds(g * block, block)
        fold_low[:, lanes] = lax.rem(index, 128)
        fold_high[:, lanes] = index // 128
        across = jnp.broadcast_to(graph_ids[pl.ds(tensor * blocks + g, 1), :], (block, block))
        down = folded(jnp.transpose(across))
        fold_same[:, lanes] = jnp.where(down == across[:fold], 1, 0)

    bias_cols[...] = jnp.transpose(bias)
    act_rows = act[...]
    for k in range(3):
        part = against_cols(weights[k], act_rows)
        if k != 1:
            column = 0 if k == 0 else 1
            part = part + bias_cols[:, column : column + 1]
        qkv[k] = part

    def head_rows(h):
        return pl.ds(pl.multiple_of(h * head_dim, 8), head_dim)

    def forward(h, carry):
        for g in range(blocks):
            lanes = pl.ds(g * block, block)
            q = qkv[0, head_rows(h), lanes].astype(bf)
            k = qkv[1, head_rows(h), lanes].astype(bf)
            v = qkv[2, head_rows(h), lanes].astype(bf)
            raw = folded(transposed_left(k, q))
            low = fold_low[:, lanes]
            high = fold_high[:, lanes]
            looked = None
            for c in range(lookups):
                source = jnp.broadcast_to(table[h, pl.ds(c, 1), :], (fold, 128))
                found = jnp.take_along_axis(source, low, axis=1, mode="promise_in_bounds")
                looked = found if c == 0 else jnp.where(high == c, found, looked)
            scores = jnp.where(fold_same[:, lanes] == 1, raw * scale + looked, masked_score)
            shifted = jnp.exp(scores - jnp.max(scores, axis=0, keepdims=True))
            part = shifted * (1.0 / jnp.sum(shifted, axis=0, keepdims=True))
            soft[g * heads + h] = part
            mixed[head_rows(h), lanes] = plain(v, unfolded(part))
        return carry

    lax.fori_loop(0, heads, forward, 0, unroll=2)

    mixed_low = mixed[...].astype(bf)
    residual[...] = embedded[...] + transposed_left(mixed_low, weights[3]) + out_bias
    again, inverse2 = normalized(residual[...])
    second[...] = again
    act2[...] = (again * gain2 + shift2).astype(bf)
    pre_act[...] = against_cols(act2[...], weights[4]) + bias[2:3]
    upward = pre_act[...]
    bell = 0.5 * (1.0 + lax.erf(upward * (1.0 / math.sqrt(2.0))))
    hidden = (upward * bell).astype(bf)
    layer_out[...] = (residual[...] + plain(hidden, weights[5]) + ffn_bias).astype(bf)
    grad_low = out_grad[...]
    hidden_grad = against_cols(grad_low, weights[5])
    slope = bell + upward * jnp.exp(-0.5 * upward * upward) * (1.0 / math.sqrt(2.0 * math.pi))
    pre_grad = (hidden_grad * slope).astype(bf)

    part = grads.shape[-2]

    def keep(target, matrix, rows_each):
        low = matrix.astype(bf)
        for p in range(planes):
            for a in range(2):
                for b in range(2):
                    at = ((p * 2 + a) * 2 + b) * rows_each
                    for c in range(2):
                        target[c, a, b, p] = low[at : at + rows_each, c * half : (c + 1) * half]

    keep(grads.at[5], transposed_left(hidden, grad_low), part)
    keep(grads.at[4], transposed_left(pre_grad, act2[...]), part)
    small[...] = jnp.zeros_like(small)

    def note(row, values):
        small[pl.ds(heads + row, 1), :] = values

    def down_sum(values):
        return jnp.sum(values, axis=0, keepdims=True)

    note(2, down_sum(pre_grad.astype(f32)))
    upstream = grad_low.astype(f32)
    note(6, down_sum(upstream))
    normed2_grad = plain(pre_grad, weights[4])

    def norm_through(grad, unit, inverse, gain):
        scaled = grad * gain
        first_mean = jnp.mean(scaled, axis=1, keepdims=True)
        second_mean = jnp.mean(scaled * unit, axis=1, keepdims=True)
        return inverse * (scaled - first_mean - unit * second_mean)

    note(7, down_sum(normed2_grad * second[...]))
    note(8, down_sum(normed2_grad))
    residual_grad = upstream + norm_through(normed2_grad, second[...], inverse2, gain2)
    residual[...] = residual_grad
    note(3, down_sum(residual_grad))
    attn_grad = residual_grad.astype(bf)
    keep(grads.at[3], plain(mixed_low, attn_grad), part)
    mixed_grad[...] = against_cols(weights[3], attn_grad)

    def backward(h, carry):
        for g in range(blocks):
            lanes = pl.ds(g * block, block)
            q = qkv[0, head_rows(h), lanes].astype(bf)
            k = qkv[1, head_rows(h), lanes].astype(bf)
            v = qkv[2, head_rows(h), lanes].astype(bf)
            d = mixed_grad[head_rows(h), lanes].astype(bf)
            probs = soft[g * heads + h]
            weighted = probs * folded(transposed_left(v, d))
            change = weighted - probs * jnp.sum(weighted, axis=0, keepdims=True)
            change_low = change.astype(bf).astype(f32)
            scores_grad[g, pl.ds(h, fold, stride=heads), :] = change_low
            change_full = unfolded(change_low)
            stacked[0, head_rows(h), lanes] = plain(k, change_full) * scale
            stacked[1, head_rows(h), lanes] = against_cols(q, change_full) * scale
            stacked[2, head_rows(h), lanes] = against_cols(d, unfolded(probs))
        return carry

    lax.fori_loop(0, heads, backward, 0, unroll=2)

    def tally(j, total):
        change = jnp.concatenate(
            [scores_grad[g, pl.ds(pl.multiple_of(j * heads, 8), heads), :] for g in range(blocks)],
            axis=1,
        )
        low = fold_low[pl.ds(j, 1), :]
        high = fold_high[pl.ds(j, 1), :]
        picked = jnp.concatenate(
            [jnp.where(high == c, change, 0.0) for c in range(lookups)], axis=0
        ).astype(bf)
        mark = (lax.broadcasted_iota(jnp.int32, (128, rows), 0) == low).astype(f32).astype(bf)
        return total + against_cols(picked, mark)

    tallied = lax.fori_loop(
        0, fold, tally, jnp.zeros((lookups * heads, 128), f32), unroll=2
    )
    for c in range(lookups):
        small[pl.ds(0, heads), pl.ds(c * 128, 128)] = tallied[c * heads : (c + 1) * heads]

    normed1_grad = None
    for k in range(3):
        low = stacked[k].astype(bf)
        if k != 1:
            note(0 if k == 0 else 1, down_sum(jnp.transpose(low.astype(f32))))
        keep(grads.at[k], plain(low, act_rows), part)
        piece = transposed_left(low, weights[k])
        normed1_grad = piece if k == 0 else normed1_grad + piece
    note(4, down_sum(normed1_grad * normed[...]))
    note(5, down_sum(normed1_grad))
    embedded_grad = residual[...] + norm_through(normed1_grad, normed[...], inverse1, gain1)
    embedded_low = embedded_grad.astype(bf)
    input_grad[...] = embedded_low
    keep(table_grad, plain(onehot, embedded_low), table_grad.shape[-2])
    small_out[...] = small[...].astype(bf)


def run_layer(
    planes, heads, features, graph_ids, degree, distance, out_grad, weights, tables, biases, vectors, degree_table
):
    rows, width = features.shape
    block = graph_ids.shape[1]
    blocks = rows // block
    half = width // 2
    part = width // (planes * 4)
    table_part = degree_table.shape[0] // (planes * 4)
    small_rows = -(-(heads + 9) // 16) * 16
    bf, f32 = jnp.bfloat16, jnp.float32
    vmem = pl.BlockSpec(memory_space=pltpu.VMEM)
    return pl.pallas_call(
        functools.partial(layer_kernel, (planes, heads, width // heads, block, half)),
        out_shape=(
            jax.ShapeDtypeStruct((rows, width), bf),
            jax.ShapeDtypeStruct((rows, width), bf),
            jax.ShapeDtypeStruct((WEIGHTS, 2, 2, 2, planes, part, half), bf),
            jax.ShapeDtypeStruct((2, 2, 2, planes, table_part, half), bf),
            jax.ShapeDtypeStruct((small_rows, width), bf),
        ),
        in_specs=[vmem] * 15,
        out_specs=(vmem,) * 5,
        scratch_shapes=[
            pltpu.VMEM((rows, width), f32),
            pltpu.VMEM((rows, width), f32),
            pltpu.VMEM((rows, width), bf),
            pltpu.VMEM((3, width, rows), f32),
            pltpu.VMEM((width, rows), f32),
            pltpu.VMEM((blocks * heads, block // 2, block), f32),
            pltpu.VMEM((blocks, block // 2 * heads, block), f32),
            pltpu.VMEM((block // 2, rows), jnp.int32),
            pltpu.VMEM((block // 2, rows), jnp.int32),
            pltpu.VMEM((block // 2, rows), jnp.int32),
            pltpu.VMEM((rows, width), f32),
            pltpu.VMEM((rows, width), f32),
            pltpu.VMEM((rows, width), bf),
            pltpu.VMEM((width, rows), f32),
            pltpu.VMEM((3, width, rows), f32),
            pltpu.VMEM((rows, width), f32),
            pltpu.VMEM((width, 8), f32),
            pltpu.VMEM((heads, tables.shape[2] // 128, 128), f32),
            pltpu.VMEM((small_rows, width), f32),
        ],
        name="layer",
    )(features, graph_ids, degree, distance, out_grad, weights, tables, biases, *vectors, degree_table)


def finish_kernel(
    shape,
    fin,
    fin_table,
    total,
    qkv_out,
    qv_out,
    out_w_out,
    ffn_in_out,
    ffn_in_b_out,
    ffn_out_out,
    table_out,
    spatial_out,
    *vector_outs,
):
    planes, heads, local_width = shape
    part, half = fin.shape[-2:]
    table_part = fin_table.shape[-2]
    f32 = jnp.float32
    tensor = lax.axis_index("tensor")
    targets = [qkv_out.at[0], qkv_out.at[1], qkv_out.at[2], out_w_out, ffn_in_out, ffn_out_out]
    for c in range(2):
        lanes = pl.ds(c * half, half)
        for a in range(2):
            for b in range(2):
                at = pl.ds((a * 2 + b) * part, part)
                for w, target in enumerate(targets):
                    target[at, lanes] = fin[w, c, a, b].astype(f32)
                for p in range(planes):
                    at_table = pl.ds(((p * 2 + a) * 2 + b) * table_part, table_part)
                    table_out[at_table, lanes] = fin_table[c, a, b, p].astype(f32)
    local_heads = heads // planes
    spatial_out[...] = total[
        pl.ds(pl.multiple_of(tensor * local_heads, 8), local_heads), pl.ds(0, spatial_out.shape[1])
    ]
    rows = total[pl.ds(heads, 16), :]
    own = rows[:, :local_width]
    for p in range(1, planes):
        own = jnp.where(tensor == p, rows[:, p * local_width : (p + 1) * local_width], own)
    qv_out[...] = own[:2]
    ffn_in_b_out[...] = own[2]
    for n, target in enumerate(vector_outs):
        target[...] = rows[3 + n]


def finish(planes, heads, local_width, degrees, table_rows, fin, fin_table, total):
    width = total.shape[1]
    f32 = jnp.float32
    vmem = pl.BlockSpec(memory_space=pltpu.VMEM)
    matrix = jax.ShapeDtypeStruct((local_width, width), f32)
    return pl.pallas_call(
        functools.partial(finish_kernel, (planes, heads, local_width)),
        out_shape=(
            jax.ShapeDtypeStruct((3, local_width, width), f32),
            jax.ShapeDtypeStruct((2, local_width), f32),
            matrix,
            matrix,
            jax.ShapeDtypeStruct((local_width,), f32),
            matrix,
            jax.ShapeDtypeStruct((degrees, width), f32),
            jax.ShapeDtypeStruct((heads // planes, table_rows), f32),
        )
        + (jax.ShapeDtypeStruct((width,), f32),) * 6,
        in_specs=[vmem] * 3,
        out_specs=(vmem,) * 14,
        name="finish",
    )(fin, fin_table, total)


def shards(
    planes,
    groups,
    node_features,
    graph_ids,
    degree,
    distance,
    out_grad,
    qkv_weight,
    qv_bias,
    out_weight,
    out_bias,
    norm1_gain,
    norm1_shift,
    ffn_in_weight,
    ffn_in_bias,
    ffn_out_weight,
    ffn_out_bias,
    norm2_gain,
    norm2_shift,
    degree_table,
    spatial_table,
):
    tensor = lax.axis_index("tensor")
    rows = node_features.shape[0]
    local_width = qkv_weight.shape[1]
    width = qkv_weight.shape[2]
    heads = spatial_table.shape[0] * planes
    table_rows = spatial_table.shape[1]

    bias_pack = jnp.pad(jnp.concatenate([qv_bias, ffn_in_bias[None]], axis=0), ((0, 5), (0, 0)))
    weights, tables, biases = gather_weights(
        planes, qkv_weight, out_weight, ffn_in_weight, ffn_out_weight, spatial_table, bias_pack
    )
    layer_out, input_grad, grads, degree_grad, small = run_layer(
        planes,
        heads,
        node_features,
        graph_ids,
        degree.reshape(1, rows),
        distance,
        out_grad,
        weights,
        tables,
        biases,
        (out_bias, norm1_gain, norm1_shift, ffn_out_bias, norm2_gain, norm2_shift),
        degree_table,
    )
    fin, fin_table, total = reduce_all(
        planes, groups, grads, degree_grad, small
    )

    finished = finish(planes, heads, local_width, degree_table.shape[0], table_rows, fin, fin_table, total)
    qkv_out, qv_out, out_w_out, ffn_in_out, ffn_in_b_out, ffn_out_out, table_out, spatial_out = finished[:8]
    out_b_out, gain1_out, shift1_out, ffn_b_out, gain2_out, shift2_out = finished[8:]
    return (
        layer_out,
        input_grad,
        qkv_out,
        qv_out,
        out_w_out,
        out_b_out,
        gain1_out,
        shift1_out,
        ffn_in_out,
        ffn_in_b_out,
        ffn_out_out,
        ffn_b_out,
        gain2_out,
        shift2_out,
        table_out,
        spatial_out,
    )


def solution(mesh):
    planes = mesh.shape["tensor"]
    groups = mesh.shape["dp"] // 8
    return jax.shard_map(
        functools.partial(shards, planes, groups),
        mesh=mesh,
        in_specs=(
            P(("dp", "tensor"), None),
            P("dp", None),
            P(("dp", "tensor")),
            P("dp", None),
            P(("dp", "tensor"), None),
            P(None, "tensor", None),
            P(None, "tensor"),
            P("tensor", None),
            P(),
            P(),
            P(),
            P("tensor", None),
            P("tensor"),
            P("tensor", None),
            P(),
            P(),
            P(),
            P(),
            P("tensor", None),
        ),
        out_specs=(
            P(("dp", "tensor"), None),
            P(("dp", "tensor"), None),
            P(None, "tensor", None),
            P(None, "tensor"),
            P("tensor", None),
            P(),
            P(),
            P(),
            P("tensor", None),
            P("tensor"),
            P("tensor", None),
            P(),
            P(),
            P(),
            P(),
            P("tensor", None),
        ),
        check_vma=False,
    )
```
